128 devices in a mesh: section: 4 (over z), dp: 16 (over y_lo, x, core), mp: 2 (over y_hi).
Axes of the slice: x: 4, y: 4 (y_hi: 2, y_lo: 2; y = y_hi * 2 + y_lo), z: 4, core: 2. Of those that a mesh axis runs over, the one named last changes fastest.
Arguments:
- tokens: bfloat16 [3, 64, 4096], P(None, ('dp', 'mp')), may hold values from -6 to 6
- member_ids: int32 [3, 64], replicated, may hold values from 0 to 3
- cotangent: bfloat16 [3, 64, 4096], P(None, ('dp', 'mp')), may hold values from -6 to 6
- w_gate: bfloat16 [4, 4096, 14336], P('section', None, ('dp', 'mp')), may hold values from -0.09375 to 0.09375
- w_up: bfloat16 [4, 4096, 14336], P('section', None, ('dp', 'mp')), may hold values from -0.09375 to 0.09375
- w_down: bfloat16 [4, 14336, 4096], P('section', ('dp', 'mp')), may hold values from -0.046875 to 0.046875
- in_scale: float32 [4, 4, 4096], P('section'), may hold values from 0.5 to 1.5
- mid_scale: float32 [4, 4, 14336], P('section', None, ('dp', 'mp')), may hold values from 0.5 to 1.5
- out_scale: float32 [4, 4, 4096], P('section'), may hold values from 0.5 to 1.5
- norm_gain: float32 [4, 4096], P('section'), may hold values from 0.5 to 1.5
Outputs:
- layer_outputs: bfloat16 [4, 3, 64, 4096], P('section', None, ('dp', 'mp'))
- section_in_grads: bfloat16 [4, 3, 64, 4096], P('section', None, ('dp', 'mp'))
- grad_gate: bfloat16 [4, 4096, 14336], P('section', None, ('dp', 'mp'))
- grad_up: bfloat16 [4, 4096, 14336], P('section', None, ('dp', 'mp'))
- grad_down: bfloat16 [4, 14336, 4096], P('section', ('dp', 'mp'))
- grad_in_scale: float32 [4, 4, 4096], P('section')
- grad_mid_scale: float32 [4, 4, 14336], P('section', None, ('dp', 'mp'))
- grad_out_scale: float32 [4, 4, 4096], P('section')
- grad_gain: float32 [4, 4096], P('section')
The draws below stay inside these ranges and needn't reach their ends.
All inputs are finite; a program needn't handle non-finite values.
Results may differ from the reference program's by a relative error of at most 0.038.
Values may be sent and summed in bfloat16 or wider, within the bound.
A program may use at most 128 MiB of HBM per device.

```python
import jax
import jax.numpy as jnp
from jax import lax

D = 4096
FF = 14336
MEMBERS = 4
MICRO = 3
TOKENS_MB = 64
LAYERS = 4


def touch_ends(drawn, rng, least, top_value):
    longest = drawn.shape.index(max(drawn.shape))
    spots = []
    for shift in (0, 1):
        where = [jax.random.randint(jax.random.fold_in(rng, axis), (), 0, length) for axis, length in enumerate(drawn.shape)]
        where[longest] = (where[longest] + shift) % drawn.shape[longest]
        spots.append(tuple(where))
    return drawn.at[spots[0]].set(least).at[spots[1]].set(top_value)


def levels(key, shape, cuts, least, top_value):
    factor_of, own = 1.0, jax.random.fold_in(key, 6)
    for axis_at, blocks in cuts:
        draws = jnp.exp(jax.random.uniform(jax.random.fold_in(own, axis_at), (blocks,), jnp.float32, least / len(cuts), top_value / len(cuts)))
        factor_of = factor_of * jnp.repeat(draws, shape[axis_at] // blocks).reshape([-1 if axis == axis_at else 1 for axis in range(len(shape))])
    return factor_of


def bell_draw(key, dims, spread, reach, cuts=(), kind=jnp.bfloat16):
    result = jax.random.normal(key, dims, jnp.float32) * spread
    if len(cuts) > 0:
        result = levels(key, dims, cuts, -0.22, 0.18) * result
    return jnp.clip(result, min=-reach, max=reach).astype(kind)


def setup_inputs(seed: int = 0) -> dict:
    arg_keys = jax.random.split(jax.random.key(seed), 11)
    return {
        "tokens": bell_draw(arg_keys[0], (MICRO, TOKENS_MB, D), 1.0, 6.0, ((1, 32),)),
        "member_ids": touch_ends(jax.random.randint(arg_keys[1], (MICRO, TOKENS_MB), 0, MEMBERS), jax.random.fold_in(arg_keys[1], 1), 0, MEMBERS - 1).astype(jnp.int32),
        "cotangent": bell_draw(arg_keys[2], (MICRO, TOKENS_MB, D), 1.0, 6.0, ((1, 32),)),
        "w_gate": bell_draw(arg_keys[3], (LAYERS, D, FF), D ** -0.5, 0.09375, ((0, 4), (2, 32))),
        "w_up": bell_draw(arg_keys[4], (LAYERS, D, FF), D ** -0.5, 0.09375, ((0, 4), (2, 32))),
        "w_down": bell_draw(arg_keys[5], (LAYERS, FF, D), FF ** -0.5, 0.046875, ((0, 4), (1, 32))),
        "in_scale": jnp.clip(0.5 + 1.0 * jax.random.uniform(arg_keys[6], (LAYERS, MEMBERS, D), jnp.float32) ** levels(arg_keys[6], (LAYERS, MEMBERS, D), ((0, 4),), -0.2, 0.2), 0.5, 1.5),
        "mid_scale": jnp.clip(0.5 + 1.0 * jax.random.uniform(arg_keys[7], (LAYERS, MEMBERS, FF), jnp.float32) ** levels(arg_keys[7], (LAYERS, MEMBERS, FF), ((0, 4), (2, 32)), -0.2, 0.2), 0.5, 1.5),
        "out_scale": jnp.clip(0.5 + 1.0 * jax.random.uniform(arg_keys[8], (LAYERS, MEMBERS, D), jnp.float32) ** levels(arg_keys[8], (LAYERS, MEMBERS, D), ((0, 4),), -0.2, 0.2), 0.5, 1.5),
        "norm_gain": jnp.clip(1.0 + 0.1 * jax.random.normal(arg_keys[9], (LAYERS, D), jnp.float32), 0.5, 1.5),
    }


EPS = 1e-05
HIGH = lax.Precision.HIGHEST

def member_table(onehot, table):
    return jnp.dot(onehot, table, precision=HIGH)

def member_sums(onehot, values):
    return jnp.dot(onehot.T, values, precision=HIGH)

def contract_rows(left, right):
    return lax.dot_general(left, right, (((0,), (0,)), ((), ())), preferred_element_type=jnp.float32)

def contract_cols(left, right):
    return lax.dot_general(left, right, (((1,), (1,)), ((), ())), preferred_element_type=jnp.float32)

def reference(tokens, member_ids, cotangent, w_gate, w_up, w_down, in_scale, mid_scale, out_scale, norm_gain):
    layers = w_gate.shape[0]
    micro = tokens.shape[0]
    members = in_scale.shape[1]
    labels = jnp.arange(members, dtype=jnp.int32)
    hots = [(member_ids[k][:, None] == labels[None, :]).astype(jnp.float32) for k in range(micro)]
    saved = {}
    layer_outs = []
    for layer in range(layers):
        outs_here = []
        for k in range(micro):
            current = tokens[k] if layer == 0 else layer_outs[layer - 1][k]
            onehot = hots[k]
            x_float = current.astype(jnp.float32)
            inv_rms = lax.rsqrt(lax.optimization_barrier(jnp.mean(x_float * x_float, axis=-1, keepdims=True)) + EPS)
            normed = x_float * inv_rms
            scaled = (normed * norm_gain[layer] * member_table(onehot, in_scale[layer])).astype(jnp.bfloat16)
            gate_pre = jnp.dot(scaled, w_gate[layer], preferred_element_type=jnp.float32)
            up_pre = jnp.dot(scaled, w_up[layer], preferred_element_type=jnp.float32)
            product = jax.nn.silu(gate_pre) * up_pre
            hidden = (product * member_table(onehot, mid_scale[layer])).astype(jnp.bfloat16)
            down_out = jnp.dot(hidden, w_down[layer], preferred_element_type=jnp.float32)
            x_next = (x_float + down_out * member_table(onehot, out_scale[layer])).astype(jnp.bfloat16)
            saved[layer, k] = (x_float, inv_rms, normed, scaled, gate_pre, up_pre, product, hidden, down_out)
            outs_here.append(x_next)
        layer_outs.append(outs_here)
    grads_in = [None] * layers
    gates_acc, ups_acc, downs_acc = ([], [], [])
    in_acc, mid_acc, out_acc, gain_acc = ([], [], [], [])
    upper = [cotangent[k] for k in range(micro)]
    for layer in reversed(range(layers)):
        acc_gate = jnp.zeros(w_gate.shape[1:], jnp.float32)
        acc_up = jnp.zeros(w_up.shape[1:], jnp.float32)
        acc_down = jnp.zeros(w_down.shape[1:], jnp.float32)
        acc_in = jnp.zeros(in_scale.shape[1:], jnp.float32)
        acc_mid = jnp.zeros(mid_scale.shape[1:], jnp.float32)
        acc_out = jnp.zeros(out_scale.shape[1:], jnp.float32)
        acc_gain = jnp.zeros(norm_gain.shape[1:], jnp.float32)
        lower = []
        for k in range(micro):
            onehot = hots[k]
            x_float, inv_rms, normed, scaled, gate_pre, up_pre, product, hidden, down_out = saved[layer, k]
            grad_y = upper[k].astype(jnp.float32)
            acc_out = acc_out + member_sums(onehot, grad_y * down_out)
            scaled_cot = (grad_y * member_table(onehot, out_scale[layer])).astype(jnp.bfloat16)
            grad_hidden = contract_cols(scaled_cot, w_down[layer])
            acc_down = acc_down + contract_rows(hidden, scaled_cot)
            acc_mid = acc_mid + member_sums(onehot, grad_hidden * product)
            grad_product = grad_hidden * member_table(onehot, mid_scale[layer])
            sigma = jax.nn.sigmoid(gate_pre)
            grad_gate_pre = (grad_product * up_pre * sigma * (1.0 + gate_pre * (1.0 - sigma))).astype(jnp.bfloat16)
            grad_up_pre = (grad_product * gate_pre * sigma).astype(jnp.bfloat16)
            acc_gate = acc_gate + contract_rows(scaled, grad_gate_pre)
            acc_up = acc_up + contract_rows(scaled, grad_up_pre)
            grad_scaled = contract_cols(grad_gate_pre, w_gate[layer]) + contract_cols(grad_up_pre, w_up[layer])
            acc_in = acc_in + member_sums(onehot, grad_scaled * normed * norm_gain[layer])
            grad_w = grad_scaled * member_table(onehot, in_scale[layer])
            acc_gain = acc_gain + lax.optimization_barrier(jnp.sum(grad_w * normed, axis=0))
            grad_normed = grad_w * norm_gain[layer]
            grad_x = inv_rms * (grad_normed - normed * lax.optimization_barrier(jnp.mean(grad_normed * normed, axis=-1, keepdims=True)))
            lower.append((grad_y + grad_x).astype(jnp.bfloat16))
        grads_in[layer] = jnp.stack(lower)
        upper = lower
        gates_acc.insert(0, acc_gate.astype(jnp.bfloat16))
        ups_acc.insert(0, acc_up.astype(jnp.bfloat16))
        downs_acc.insert(0, acc_down.astype(jnp.bfloat16))
        in_acc.insert(0, acc_in)
        mid_acc.insert(0, acc_mid)
        out_acc.insert(0, acc_out)
        gain_acc.insert(0, acc_gain)
    layer_outputs = jnp.stack([jnp.stack(layer_outs[layer]) for layer in range(layers)])
    return (layer_outputs, jnp.stack(grads_in), jnp.stack(gates_acc), jnp.stack(ups_acc), jnp.stack(downs_acc), jnp.stack(in_acc), jnp.stack(mid_acc), jnp.stack(out_acc), jnp.stack(gain_acc))
```

```python
import functools

import jax
import jax.numpy as jnp
from jax import lax
from jax.experimental import pallas as pl
from jax.experimental.pallas import tpu as pltpu
from jax.sharding import PartitionSpec as P

EPS = 1e-05
F32 = jnp.float32
BF16 = jnp.bfloat16


def nt_dot(left, right):
    return lax.dot_general(left, right, (((1,), (1,)), ((), ())), preferred_element_type=F32)


def pick(table, ids, members):
    rows = ids.shape[0]
    value = jnp.broadcast_to(table[members - 1 : members], (rows, table.shape[1]))
    for m in range(members - 1):
        value = jnp.where(ids == m, table[m : m + 1], value)
    return value


def relay_kernel(
    dims,
    tok, cot, ids, wg_h, wu_h, wd_h, in_tab, gain, out_tab, mid_tab,
    out, hid, dg, du, sc, ct, gtab, gmid,
    wg, wu, wd, sel, t1, initr, rowf, xin, gin, xg, gg, gt_tab, inv, gpre, upre,
    psend, precv, pown, pf, rbuf, csend, cprecv, cown, crbuf, down, ob, ig,
    acc_in, acc_out, gtl, outs, outr, outp,
    wsem, isem, zs, zr, ags, agr, ds, dr, ps, pr, rs, rr, cps, cpr, cs, cr, osem,
):
    sections, chips, micro, rows, members = dims
    width = in_tab.shape[1]
    hidden = mid_tab.shape[1]
    half = width // 2
    bw = half // chips
    total = rows * 2 * chips
    s = lax.axis_index("section")
    dp = lax.axis_index("dp")
    mp = lax.axis_index("mp")
    mps = lax.axis_size("mp")
    core = lax.rem(dp, 2)
    other = 1 - core
    q = (dp // 2) * mps + mp
    block = core * chips + q
    last = sections - 1
    partner = {"dp": (dp // 2) * 2 + other, "mp": mp}
    above = {"section": jnp.minimum(s + 1, last)}
    below = {"section": jnp.maximum(s - 1, 0)}

    def chip(j):
        to = lax.rem(q + j, chips)
        return to, {"dp": (to // mps) * 2 + core, "mp": lax.rem(to, mps)}

    def remote(src, dst, send, recv, device):
        return pltpu.make_async_remote_copy(
            src_ref=src, dst_ref=dst, send_sem=send, recv_sem=recv,
            device_id=device, device_id_type=pl.DeviceIdType.MESH,
        )

    def cols(index, size):
        return pl.ds(pl.multiple_of(index * size, size), size)

    weights = [
        pltpu.make_async_copy(h, v, wsem.at[i])
        for i, (h, v) in enumerate(((wg_h, wg), (wu_h, wu), (wd_h, wd)))
    ]
    for copy in weights:
        copy.start()

    barrier = pltpu.get_barrier_semaphore()
    for j in range(1, chips):
        pl.semaphore_signal(barrier, inc=1, device_id=chip(j)[1], device_id_type=pl.DeviceIdType.MESH)
    pl.semaphore_signal(barrier, inc=1, device_id=partner, device_id_type=pl.DeviceIdType.MESH)

    @pl.when(s < last)
    def _():
        pl.semaphore_signal(barrier, inc=1, device_id=above, device_id_type=pl.DeviceIdType.MESH)

    @pl.when(s > 0)
    def _():
        pl.semaphore_signal(barrier, inc=1, device_id=below, device_id_type=pl.DeviceIdType.MESH)

    @pl.when(s == 0)
    def _():
        sel[...] = tok[...]

    @pl.when(s > 0)
    def _():
        sel[...] = cot[...]

    gt_tab[...] = in_tab[...] * gain[...]
    acc_in[...] = jnp.zeros_like(acc_in)
    acc_out[...] = jnp.zeros_like(acc_out)
    gmid[...] = jnp.zeros_like(gmid)
    gtl[...] = jnp.zeros_like(gtl)
    pl.semaphore_wait(barrier, chips + (s < last).astype(jnp.int32) + (s > 0).astype(jnp.int32))

    mine = pl.ds(core * micro, micro)
    first = remote(sel.at[:, :, cols(other, half)], t1.at[mine], isem.at[0], isem.at[1], partner)
    first.start()
    t1[mine] = sel[:, :, cols(core, half)]
    first.wait_recv()
    for j in range(1, chips):
        to, device = chip(j)
        remote(t1.at[:, :, cols(to, bw)], initr.at[q], isem.at[2], isem.at[3], device).start()
    initr[q] = t1[:, :, cols(q, bw)]
    others = initr.at[pl.ds(0, chips - 1)]
    second = remote(others, others, isem.at[2], isem.at[3], partner)
    second.wait_recv()
    for k in range(micro):
        for i in range(chips):
            for c in range(2):
                at = (i * 2 + c) * rows
                rowf[at : at + rows, :] = initr[i, c * micro + k].astype(F32)

        @pl.when(s == 0)
        def _():
            xin[k] = rowf[...].astype(BF16)

        @pl.when(s == last)
        def _():
            gin[k] = rowf[...].astype(BF16)

    for copy in weights:
        copy.wait()

    my_cols = cols(block, bw)
    core_cols = cols(core, half)
    r15 = lambda ph, k: rbuf.at[ph, k, pl.ds(0, chips - 1)]

    def spread(ph, k, src, dst):
        dst[k, :, my_cols] = src[k]
        for j in range(1, chips):
            remote(src.at[k], dst.at[k, :, my_cols], ags.at[ph, k], agr.at[ph, k], chip(j)[1]).start()

    def gather_rest(ph, k, dst):
        remote(r15(ph, k), r15(ph, k), ags.at[ph, k], agr.at[ph, k], partner).wait_recv()
        part = dst.at[k, :, core_cols]
        copy = remote(part, part, ds.at[ph, k], dr.at[ph, k], partner)
        copy.start()
        copy.wait_recv()

    def reduce_out(ph, k, term):
        step = min(512, half)
        each = step // bw
        for n in range(half // step):
            value = term(pl.ds(pl.multiple_of(other * half + n * step, step), step))
            for e in range(each):
                psend[ph, k, n * each + e] = value[:, e * bw : (e + 1) * bw].astype(BF16)
        copy = remote(psend.at[ph, k], precv.at[ph, k], ps.at[ph, k], pr.at[ph, k], partner)
        copy.start()
        for n in range(half // step):
            value = term(pl.ds(pl.multiple_of(core * half + n * step, step), step))
            for e in range(each):
                pf[n * each + e] = value[:, e * bw : (e + 1) * bw]
        copy.wait_recv()
        for n in range(chips):
            pown[ph, k, n] = (pf[n] + precv[ph, k, n].astype(F32)).astype(BF16)
        for j in range(1, chips):
            to, device = chip(j)
            remote(pown.at[ph, k, to], rbuf.at[ph, k, q], rs.at[ph, k], rr.at[ph, k], device).start()
        rbuf[ph, k, q] = pown[ph, k, q]

    def reduced(ph, k):
        remote(r15(ph, k), r15(ph, k), rs.at[ph, k], rr.at[ph, k], partner).wait_recv()
        value = rbuf[ph, k, 0].astype(F32)
        for n in range(1, chips):
            value = value + rbuf[ph, k, n].astype(F32)
        return value

    chunk = min(512, width)
    pieces = [(at, min(256, hidden - at)) for at in range(0, hidden, 256)]

    def token_rows(k):
        return pl.ds(pl.multiple_of(k * total, total), total)

    def fwd_arrive(k):
        @pl.when(s > 0)
        def _():
            remote(xin.at[k], xin.at[k], zs.at[0, k], zr.at[0, k], above).wait_recv()

        spread(0, k, xin, xg)

    def fwd_compute(k):
        gather_rest(0, k, xg)
        here = token_rows(k)
        id_col = ids[k]
        squares = jnp.zeros((total, 128), F32)
        for n in range(width // 128):
            x = xg[k, :, n * 128 : (n + 1) * 128].astype(F32)
            squares = squares + x * x
        scale = lax.rsqrt(jnp.sum(squares, axis=-1, keepdims=True) * (1.0 / width) + EPS)
        inv[k] = scale

        def scale_chunk(n, carry):
            at = cols(n, chunk)
            x = xg[k, :, at].astype(F32)
            sc[here, at] = (x * scale * pick(gt_tab[:, at], id_col, members)).astype(BF16)
            return carry

        lax.fori_loop(0, width // chunk, scale_chunk, 0)
        for at, size in pieces:
            hs = slice(at, at + size)
            gate = nt_dot(wg[hs, :], sc[here, :]).T
            up = nt_dot(wu[hs, :], sc[here, :]).T
            gpre[k, :, hs] = gate
            upre[k, :, hs] = up
            product = gate / (1.0 + jnp.exp(-gate)) * up
            hid[here, hs] = (product * pick(mid_tab[:, hs], id_col, members)).astype(BF16)
        h = hid[here, :]
        reduce_out(0, k, lambda at: jnp.dot(h, wd[:, at], preferred_element_type=F32))

    def fwd_finish(k):
        value = reduced(0, k)
        down[k] = value
        x = xg[k, :, my_cols].astype(F32)
        ob[k] = (x + value * pick(out_tab[:, my_cols], ids[k], members)).astype(BF16)

        @pl.when(s < last)
        def _():
            remote(ob.at[k], xin.at[k], zs.at[0, k], zr.at[0, k], above).start()

    def bwd_arrive(k):
        @pl.when(s < last)
        def _():
            remote(gin.at[k], gin.at[k], zs.at[1, k], zr.at[1, k], below).wait_recv()

        spread(1, k, gin, gg)

    def bwd_compute(k):
        gather_rest(1, k, gg)
        here = token_rows(k)
        id_col = ids[k]

        def cot_chunk(n, carry):
            at = cols(n, chunk)
            g = gg[k, :, at].astype(F32)
            ct[here, at] = (g * pick(out_tab[:, at], id_col, members)).astype(BF16)
            return carry

        lax.fori_loop(0, width // chunk, cot_chunk, 0)
        dots = jnp.zeros((total, 1), F32)
        for at, size in pieces:
            hs = slice(at, at + size)
            grad_hidden = nt_dot(wd[hs, :], ct[here, :]).T
            gate = gpre[k, :, hs]
            up = upre[k, :, hs]
            sig = 1.0 / (1.0 + jnp.exp(-gate))
            silu = gate * sig
            mids = grad_hidden * (silu * up)
            for m in range(members):
                gmid[m : m + 1, hs] += jnp.sum(jnp.where(id_col == m, mids, 0.0), axis=0, keepdims=True)
            grad_product = grad_hidden * pick(mid_tab[:, hs], id_col, members)
            grad_gate = (grad_product * up * sig * (1.0 + gate * (1.0 - sig))).astype(BF16)
            grad_up = (grad_product * silu).astype(BF16)
            dg[here, hs] = grad_gate
            du[here, hs] = grad_up
            dots = dots + jnp.sum(
                grad_gate.astype(F32) * gate + grad_up.astype(F32) * up, axis=-1, keepdims=True
            )
        csend[k] = jnp.broadcast_to(dots, (total, 128)).T[0:8, :]
        ccopy = remote(csend.at[k], cprecv.at[k], cps.at[k], cpr.at[k], partner)
        ccopy.start()
        grad_gates = dg[here, :]
        grad_ups = du[here, :]

        def term(at):
            return jnp.dot(grad_gates, wg[:, at], preferred_element_type=F32) + jnp.dot(
                grad_ups, wu[:, at], preferred_element_type=F32
            )

        reduce_out(1, k, term)
        ccopy.wait_recv()
        cown[k] = csend[k] + cprecv[k]
        for j in range(1, chips):
            remote(cown.at[k], crbuf.at[k, q], cs.at[k], cr.at[k], chip(j)[1]).start()
        crbuf[k, q] = cown[k]

    def bwd_finish(k):
        id_col = ids[k]
        g = gin[k].astype(F32)
        grad_scaled = reduced(1, k)
        c15 = crbuf.at[k, pl.ds(0, chips - 1)]
        remote(c15, c15, cs.at[k], cr.at[k], partner).wait_recv()
        dots = crbuf[k, 0]
        for n in range(1, chips):
            dots = dots + crbuf[k, n]
        mean = dots.T[:, 0:1] * (1.0 / width)
        scale = inv[k]
        normed = xg[k, :, my_cols].astype(F32) * scale
        outs_here = g * down[k]
        ins_here = grad_scaled * normed
        for m in range(members):
            mask = id_col == m
            acc_out[m : m + 1, :] += jnp.sum(jnp.where(mask, outs_here, 0.0), axis=0, keepdims=True)
            acc_in[m : m + 1, :] += jnp.sum(jnp.where(mask, ins_here, 0.0), axis=0, keepdims=True)
        grad_normed = grad_scaled * pick(gt_tab[:, my_cols], id_col, members)
        ig[k] = (g + scale * (grad_normed - normed * mean)).astype(BF16)

        @pl.when(s > 0)
        def _():
            remote(ig.at[k], gin.at[k], zs.at[1, k], zr.at[1, k], below).start()

    def run(arrive, compute, finish):
        def tick(t, carry):
            @pl.when(t < micro)
            def _():
                arrive(t)

            @pl.when(jnp.logical_and(t >= 1, t < micro + 1))
            def _():
                compute(t - 1)

            @pl.when(t >= 2)
            def _():
                finish(t - 2)

            return carry

        lax.fori_loop(0, micro + 2, tick, 0)

    run(fwd_arrive, fwd_compute, fwd_finish)
    run(bwd_arrive, bwd_compute, bwd_finish)

    tables = acc_in[...]
    gtl[0:members, :] = tables * gain[:, my_cols]
    gtl[members : 2 * members, :] = acc_out[...]
    gtl[2 * members : 2 * members + 1, :] = jnp.sum(tables * in_tab[:, my_cols], axis=0, keepdims=True)
    gtab[:, my_cols] = gtl[...]
    for j in range(1, chips):
        remote(gtl, gtab.at[:, my_cols], osem.at[0], osem.at[1], chip(j)[1]).start()

    for kind, src in ((0, ob), (1, ig)):
        for k in range(micro):
            rowf[...] = src[k].astype(F32)
            for i in range(chips):
                for c in range(2):
                    at = (i * 2 + c) * rows
                    outs[i, (c * 2 + kind) * micro + k] = rowf[at : at + rows, :].astype(BF16)
    for j in range(1, chips):
        to, device = chip(j)
        remote(outs.at[to], outr.at[:, :, cols(q, bw)], osem.at[2], osem.at[3], device).start()
    outr[:, :, cols(q, bw)] = outs[q]

    most = gtab.at[:, pl.ds(0, (chips - 1) * bw)]
    remote(most, most, osem.at[0], osem.at[1], partner).wait_recv()
    table_part = gtab.at[:, core_cols]
    tables_on = remote(table_part, table_part, osem.at[4], osem.at[5], partner)
    tables_on.start()
    most_outs = outs.at[pl.ds(0, chips - 1)]
    remote(most_outs, most_outs, osem.at[2], osem.at[3], partner).wait_recv()
    rows_on = remote(outr.at[pl.ds(other * 2 * micro, 2 * micro)], outp, osem.at[6], osem.at[7], partner)
    rows_on.start()
    out[:, :, core_cols] = outr[pl.ds(core * 2 * micro, 2 * micro)]

    first.wait_send()
    second.wait_send()
    for ph in range(2):
        for k in range(micro):
            remote(r15(ph, k), r15(ph, k), ags.at[ph, k], agr.at[ph, k], partner).wait_send()
            remote(r15(ph, k), r15(ph, k), rs.at[ph, k], rr.at[ph, k], partner).wait_send()
            part = xg.at[k, :, core_cols]
            remote(part, part, ds.at[ph, k], dr.at[ph, k], partner).wait_send()
            remote(psend.at[ph, k], precv.at[ph, k], ps.at[ph, k], pr.at[ph, k], partner).wait_send()
    for k in range(micro):
        remote(csend.at[k], cprecv.at[k], cps.at[k], cpr.at[k], partner).wait_send()
        c15 = crbuf.at[k, pl.ds(0, chips - 1)]
        remote(c15, c15, cs.at[k], cr.at[k], partner).wait_send()

        @pl.when(s < last)
        def _():
            remote(ob.at[k], xin.at[k], zs.at[0, k], zr.at[0, k], above).wait_send()

        @pl.when(s > 0)
        def _():
            remote(ig.at[k], gin.at[k], zs.at[1, k], zr.at[1, k], below).wait_send()

    remote(most, most, osem.at[0], osem.at[1], partner).wait_send()
    remote(most_outs, most_outs, osem.at[2], osem.at[3], partner).wait_send()
    tables_on.wait()
    rows_on.wait()
    out[:, :, cols(other, half)] = outp[...]


def on_device(
    tokens, member_ids, cotangent, w_gate, w_up, w_down, in_scale, mid_scale, out_scale, norm_gain
):
    sections = lax.axis_size("section")
    mps = lax.axis_size("mp")
    places = lax.axis_size("dp") // 2
    chips = places * mps
    micro, rows, width = tokens.shape
    total = member_ids.shape[1]
    members = in_scale.shape[1]
    hidden = w_gate.shape[2]
    half = width // 2
    bw = half // chips
    ids = member_ids.reshape(micro, places, 2, mps, rows).transpose(0, 1, 3, 2, 4)
    ids = ids.reshape(micro, total, 1)
    gate_t = w_gate[0].T
    up_t = w_up[0].T
    down_w = w_down[0]
    all_tokens = micro * total
    vmem = pl.BlockSpec(memory_space=pltpu.VMEM)
    hbm = pl.BlockSpec(memory_space=pl.ANY)
    dma = pltpu.SemaphoreType.DMA

    def buf(*shape, dtype=BF16):
        return pltpu.VMEM(shape, dtype)

    dims = (sections, chips, micro, rows, members)
    outs = (
        jax.ShapeDtypeStruct((2 * micro, rows, width), BF16),
        jax.ShapeDtypeStruct((all_tokens, hidden), BF16),
        jax.ShapeDtypeStruct((all_tokens, hidden), BF16),
        jax.ShapeDtypeStruct((all_tokens, hidden), BF16),
        jax.ShapeDtypeStruct((all_tokens, width), BF16),
        jax.ShapeDtypeStruct((all_tokens, width), BF16),
        jax.ShapeDtypeStruct((16, width), F32),
        jax.ShapeDtypeStruct((members, hidden), F32),
    )
    out, hid, dg, du, sc, ct, gtab, gmid = pl.pallas_call(
        functools.partial(relay_kernel, dims),
        name="relay",
        out_shape=outs,
        in_specs=[vmem, vmem, vmem, hbm, hbm, hbm, vmem, vmem, vmem, vmem],
        out_specs=[vmem] * len(outs),
        scratch_shapes=[
            buf(hidden, width), buf(hidden, width), buf(hidden, width),
            buf(micro, rows, width),
            buf(2 * micro, rows, half),
            buf(chips, 2 * micro, rows, bw),
            buf(total, bw, dtype=F32),
            buf(micro, total, bw), buf(micro, total, bw),
            buf(micro, total, width), buf(micro, total, width),
            buf(members, width, dtype=F32),
            buf(micro, total, 1, dtype=F32),
            buf(micro, total, hidden, dtype=F32), buf(micro, total, hidden, dtype=F32),
            buf(2, micro, chips, total, bw), buf(2, micro, chips, total, bw),
            buf(2, micro, chips, total, bw),
            buf(chips, total, bw, dtype=F32),
            buf(2, micro, chips, total, bw),
            buf(micro, 8, total, dtype=F32), buf(micro, 8, total, dtype=F32),
            buf(micro, 8, total, dtype=F32), buf(micro, chips, 8, total, dtype=F32),
            buf(micro, total, bw, dtype=F32),
            buf(micro, total, bw), buf(micro, total, bw),
            buf(members, bw, dtype=F32), buf(members, bw, dtype=F32),
            buf(16, bw, dtype=F32),
            buf(chips, 4 * micro, rows, bw),
            buf(4 * micro, rows, half),
            buf(2 * micro, rows, half),
            dma((3,)), dma((4,)),
            dma((2, micro)), dma((2, micro)), dma((2, micro)), dma((2, micro)),
            dma((2, micro)), dma((2, micro)), dma((2, micro)), dma((2, micro)),
            dma((2, micro)), dma((2, micro)),
            dma((micro,)), dma((micro,)), dma((micro,)), dma((micro,)),
            dma((8,)),
        ],
        compiler_params=pltpu.CompilerParams(
            collective_id=0, has_side_effects=True, vmem_limit_bytes=56 * 1024 * 1024
        ),
    )(
        tokens, cotangent, ids, gate_t, up_t, down_w,
        in_scale[0], norm_gain, out_scale[0], mid_scale[0],
    )

    def weight_grad(left, right):
        return lax.dot_general(
            left, right, (((0,), (0,)), ((), ())), preferred_element_type=F32
        ).astype(BF16)

    return (
        out[:micro][None],
        out[micro:][None],
        weight_grad(dg, sc).T[None],
        weight_grad(du, sc).T[None],
        weight_grad(hid, ct)[None],
        gtab[:members][None],
        gmid[None],
        gtab[members : 2 * members][None],
        gtab[2 * members : 2 * members + 1],
    )


def solution(mesh):
    in_specs = (
        P(None, ("dp", "mp"), None),
        P(),
        P(None, ("dp", "mp"), None),
        P("section", None, ("dp", "mp")),
        P("section", None, ("dp", "mp")),
        P("section", ("dp", "mp"), None),
        P("section", None, None),
        P("section", None, ("dp", "mp")),
        P("section", None, None),
        P("section", None),
    )
    out_specs = (
        P("section", None, ("dp", "mp"), None),
        P("section", None, ("dp", "mp"), None),
        P("section", None, ("dp", "mp")),
        P("section", None, ("dp", "mp")),
        P("section", ("dp", "mp"), None),
        P("section", None, None),
        P("section", None, ("dp", "mp")),
        P("section", None, None),
        P("section", None),
    )
    return jax.shard_map(
        on_device, mesh=mesh, in_specs=in_specs, out_specs=out_specs, check_vma=False
    )
```

```python
import functools

import jax
import jax.numpy as jnp
from jax import lax
from jax.experimental import pallas as pl
from jax.experimental.pallas import tpu as pltpu
from jax.sharding import PartitionSpec as P

EPS = 1e-05
F32 = jnp.float32
BF16 = jnp.bfloat16


def nt_dot(left, right):
    return lax.dot_general(left, right, (((1,), (1,)), ((), ())), preferred_element_type=F32)


def pick(table, ids, members):
    rows = ids.shape[0]
    value = jnp.broadcast_to(table[members - 1 : members], (rows, table.shape[1]))
    for m in range(members - 1):
        value = jnp.where(ids == m, table[m : m + 1], value)
    return value


def relay_kernel(
    dims,
    tok, cot, ids, wg_h, wu_h, wd_h, in_tab, gain, out_tab, mid_tab,
    out_x, out_g, hid_t, dg_t, du_t, sc_h, ct_h, g_in, g_out, g_gain, gmid,
    hid, dg, du, sc, ct,
    wg, wu, wd, rg, t1, initr, rowf, xin, gin, xg, gg, gt_tab, idc, inv, pacc, phid, gpre, upre,
    psend, precv, pown, pf, rbuf, csend, cprecv, cown, crbuf, down, ob, ig,
    acc_in, acc_out, gtl, gtab, outs, outr, outp,
    wsem, hsem, isem, xs, xr, xds, xdr, zs, zr, ags, agr, ds, dr, ps, pr, rs, rr, cps, cpr, cs, cr, osem,
):
    sections, places, mps, micro, rows, members = dims
    chips = places * mps
    across = places // 2
    width = in_tab.shape[1]
    hidden = mid_tab.shape[1]
    half = width // 2
    bw = half // chips
    total = rows * 2 * chips
    s = lax.axis_index("section")
    dp = lax.axis_index("dp")
    mp = lax.axis_index("mp")
    core = lax.rem(dp, 2)
    other = 1 - core
    place = dp // 2
    along_x = lax.rem(place, across)
    y_low = place // across
    along_y = mp * 2 + y_low
    q = place * mps + mp
    block = core * chips + q
    last = sections - 1
    partner = {"dp": place * 2 + other, "mp": mp}
    up_s = jnp.minimum(s + 1, last)
    down_s = jnp.maximum(s - 1, 0)
    above = {"section": up_s}
    below = {"section": down_s}

    def hops(d):
        return min(d[0], across - d[0]) + min(d[1], 2 * mps - d[1])

    offsets = [(dx, dy) for dx in range(across) for dy in range(2 * mps) if dx or dy]
    offsets.sort(key=lambda d: -hops(d))
    reach = hops(offsets[0]) // 2

    def chip(dx, dy):
        x = lax.rem(along_x + dx, across)
        y = lax.rem(along_y + dy, 2 * mps)
        at = lax.rem(y, 2) * across + x
        return at * mps + y // 2, {"dp": at * 2 + core, "mp": y // 2}

    peers = [chip(*d) for d in offsets]
    far = [p for p, d in zip(peers, offsets) if hops(d) > reach]
    near = [p for p, d in zip(peers, offsets) if hops(d) <= reach]
    groups = [
        [p for p, d in zip(peers, offsets) if d[1] % 2 == 1],
        [p for p, d in zip(peers, offsets) if d[1] % 2 == 0],
    ]

    def remote(src, dst, send, recv, device):
        return pltpu.make_async_remote_copy(
            src_ref=src, dst_ref=dst, send_sem=send, recv_sem=recv,
            device_id=device, device_id_type=pl.DeviceIdType.MESH,
        )

    def cols(index, size):
        return pl.ds(pl.multiple_of(index * size, size), size)

    weights = [
        pltpu.make_async_copy(h, v, wsem.at[i])
        for i, (h, v) in enumerate(((wg_h, wg), (wu_h, wu), (wd_h, wd)))
    ]
    for copy in weights:
        copy.start()

    barrier = pltpu.get_barrier_semaphore()
    for _, device in peers:
        pl.semaphore_signal(barrier, inc=1, device_id=device, device_id_type=pl.DeviceIdType.MESH)
    pl.semaphore_signal(barrier, inc=1, device_id=partner, device_id_type=pl.DeviceIdType.MESH)

    @pl.when(s < last)
    def _():
        for device in [above] + [{**d, **above} for _, d in far]:
            pl.semaphore_signal(barrier, inc=1, device_id=device, device_id_type=pl.DeviceIdType.MESH)

    @pl.when(s > 0)
    def _():
        for device in [below] + [{**d, **below} for _, d in far]:
            pl.semaphore_signal(barrier, inc=1, device_id=device, device_id_type=pl.DeviceIdType.MESH)

    gt_tab[...] = in_tab[...] * gain[...]
    acc_in[...] = jnp.zeros_like(acc_in)
    acc_out[...] = jnp.zeros_like(acc_out)
    gmid[...] = jnp.zeros_like(gmid)
    gtl[...] = jnp.zeros_like(gtl)
    i = lax.broadcasted_iota(jnp.int32, (total, total), 0)
    j = lax.broadcasted_iota(jnp.int32, (total, total), 1)
    i_mp = (i // (2 * rows)) % mps
    i_core = (i // rows) % 2
    source = (((i // (2 * rows * mps)) * 2 + i_core) * mps + i_mp) * rows + i % rows
    for k in range(micro):
        picked = jnp.where(source == j, jnp.broadcast_to(ids[k : k + 1, :], (total, total)), 0)
        idc[k] = jnp.sum(picked.astype(F32), axis=1, keepdims=True).astype(jnp.int32)
    links = (s < last).astype(jnp.int32) + (s > 0).astype(jnp.int32)
    pl.semaphore_wait(barrier, chips + (1 + len(far)) * links)

    my_cols = cols(block, bw)
    core_cols = cols(core, half)
    r15 = lambda ph, k: rbuf.at[ph, k, pl.ds(0, chips - 1)]

    def spread(ph, k, src, dst, targets):
        for _, device in targets:
            remote(src.at[k], dst.at[k, :, my_cols], ags.at[ph, k], agr.at[ph, k], device).start()
        dst[k, :, my_cols] = src[k]

    def hand_on(ph, k, src, dst, gathered, section):
        remote(src.at[k], dst.at[k], zs.at[ph, k], zr.at[ph, k], section).start()
        for _, device in far:
            remote(
                src.at[k], gathered.at[k, :, my_cols], zs.at[ph, k], agr.at[ph, k], {**device, **section}
            ).start()

    row_part = lambda k, c: rg.at[pl.ds(c * chips, chips), k]

    @pl.when(s == 0)
    def _():
        for k in range(micro):
            for _, device in peers:
                remote(tok.at[k], rg.at[block, k], xs.at[k], xr.at[k], device).start()
            rg[block, k] = tok[k]

    def forward_rows(k):
        most_rows = rg.at[pl.ds(0, chips - 1), k]
        remote(most_rows, most_rows, xs.at[k], xr.at[k], partner).wait_recv()
        remote(row_part(k, core), row_part(k, core), xds.at[k], xdr.at[k], partner).start()

    def place_rows(k):
        remote(row_part(k, other), row_part(k, other), xds.at[k], xdr.at[k], partner).wait_recv()
        for c in range(2):
            for n in range(chips):
                at = (n * 2 + c) * rows
                xg[k, at : at + rows, :] = rg[c * chips + n, k]

    mine = pl.ds(core * micro, micro)
    first = remote(cot.at[:, :, cols(other, half)], t1.at[mine], isem.at[0], isem.at[1], partner)
    others = initr.at[pl.ds(0, chips - 1)]
    second = remote(others, others, isem.at[2], isem.at[3], partner)

    @pl.when(s == last)
    def _():
        first.start()
        t1[mine] = cot[:, :, cols(core, half)]
        first.wait_recv()
        for to, device in peers:
            remote(t1.at[:, :, cols(to, bw)], initr.at[q], isem.at[2], isem.at[3], device).start()
        initr[q] = t1[:, :, cols(q, bw)]
        second.wait_recv()
        for k in range(micro):
            for n in range(chips):
                for c in range(2):
                    at = (n * 2 + c) * rows
                    rowf[at : at + rows, :] = initr[n, c * micro + k].astype(F32)
            gin[k] = rowf[...].astype(BF16)
            spread(1, k, gin, gg, peers)

    for copy in weights:
        copy.wait()

    chunk = min(512, half)
    pieces = [(at, min(256, hidden - at)) for at in range(0, hidden, 256)]

    def part_cols(c, n, size):
        return pl.ds(pl.multiple_of(c * half + n * size, size), size)

    def gathered(ph, k):
        remote(r15(ph, k), r15(ph, k), ags.at[ph, k], agr.at[ph, k], partner).wait_recv()

    def reduce_out(ph, k, term, between=None):
        step = min(512, half // 2)
        each = step // bw
        halves = half // 2 // step
        copies = []
        for piece in range(2):
            low = 1 - y_low if piece == 0 else y_low
            with jax.named_scope("down_other"):
                for n in range(halves):
                    at = other * half + low * (half // 2) + n * step
                    value = term(pl.ds(pl.multiple_of(at, step), step))
                    for e in range(each):
                        to = low * (chips // 2) + n * each + e
                        psend[ph, k, to] = value[:, e * bw : (e + 1) * bw].astype(BF16)
            at = pl.ds(low * (chips // 2), chips // 2)
            copy = remote(
                psend.at[ph, k, at], precv.at[ph, k, at], ps.at[ph, k, piece], pr.at[ph, k, piece], partner
            )
            copy.start()
            copies.append(copy)
        with jax.named_scope("down_own"):
            for n in range(half // step):
                value = term(pl.ds(pl.multiple_of(core * half + n * step, step), step))
                for e in range(each):
                    pf[n * each + e] = value[:, e * bw : (e + 1) * bw]
        if between is not None:
            between()
        for piece in range(2):
            low = 1 - y_low if piece == 0 else y_low
            with jax.named_scope("partner_wait"):
                copies[piece].wait_recv()
            with jax.named_scope("combine"):
                for n in range(chips // 2):
                    at = low * (chips // 2) + n
                    pown[ph, k, at] = (pf[at] + precv[ph, k, at].astype(F32)).astype(BF16)
                for to, device in groups[piece]:
                    remote(pown.at[ph, k, to], rbuf.at[ph, k, q], rs.at[ph, k], rr.at[ph, k], device).start()
        rbuf[ph, k, q] = pown[ph, k, q]

    def reduced(ph, k):
        with jax.named_scope("reduce_wait"):
            remote(r15(ph, k), r15(ph, k), rs.at[ph, k], rr.at[ph, k], partner).wait_recv()
        value = rbuf[ph, k, 0].astype(F32)
        for n in range(1, chips):
            value = value + rbuf[ph, k, n].astype(F32)
        return value

    def token_rows(k):
        return pl.ds(pl.multiple_of(k * total, total), total)

    def fwd_arrive(k):
        with jax.named_scope("x_wait"):
            @pl.when(s > 0)
            def _():
                remote(xin.at[k], xin.at[k], zs.at[0, k], zr.at[0, k], above).wait_recv()
                spread(0, k, xin, xg, near)

            @pl.when(jnp.logical_and(s == 0, k == 0))
            def _():
                forward_rows(k)

    def fwd_compute(k):
        here = token_rows(k)
        id_col = idc[k]

        def scaled_half(c, squares):
            def step(n, carry):
                at = part_cols(c, n, chunk)
                x = xg[k, :, at].astype(F32)
                sc[here, at] = (x * pick(gt_tab[:, at], id_col, members)).astype(BF16)
                x2 = x * x
                for e in range(chunk // 128):
                    carry = carry + x2[:, e * 128 : (e + 1) * 128]
                return carry

            return lax.fori_loop(0, half // chunk, step, squares)

        part = xg.at[k, :, core_cols]
        copy = remote(part, part, ds.at[0, k], dr.at[0, k], partner)
        with jax.named_scope("gather_wait"):
            @pl.when(s > 0)
            def _():
                gathered(0, k)
                copy.start()

            @pl.when(s == 0)
            def _():
                place_rows(k)

        with jax.named_scope("gateup_own"):
            squares = scaled_half(core, jnp.zeros((total, 128), F32))
            at = core_cols
            for h, size in pieces:
                hs = slice(h, h + size)
                pacc[0, hs, :] = nt_dot(wg[hs, at], sc[here, at])
                pacc[1, hs, :] = nt_dot(wu[hs, at], sc[here, at])
        with jax.named_scope("forward_wait"):
            @pl.when(s > 0)
            def _():
                copy.wait_recv()

            @pl.when(jnp.logical_and(s == 0, k < micro - 1))
            def _():
                forward_rows(jnp.minimum(k + 1, micro - 1))

        with jax.named_scope("gateup_other"):
            squares = scaled_half(other, squares)
            scale = lax.rsqrt(jnp.sum(squares, axis=-1, keepdims=True) * (1.0 / width) + EPS)
            inv[k] = scale
            at = cols(other, half)
            for h, size in pieces:
                hs = slice(h, h + size)
                gate = (pacc[0, hs, :] + nt_dot(wg[hs, at], sc[here, at])).T * scale
                up = (pacc[1, hs, :] + nt_dot(wu[hs, at], sc[here, at])).T * scale
                gpre[k, :, hs] = gate
                upre[k, :, hs] = up
                product = gate / (1.0 + jnp.exp(-gate)) * up
                hid[here, hs] = (product * pick(mid_tab[:, hs], id_col, members)).astype(BF16)
        h = hid[here, :]
        reduce_out(0, k, lambda at: jnp.dot(h, wd[:, at], preferred_element_type=F32))

    def fwd_finish(k):
        value = reduced(0, k)
        with jax.named_scope("fwd_finish"):
            x = xg[k, :, my_cols].astype(F32)
            ob[k] = (x + value * pick(out_tab[:, my_cols], idc[k], members)).astype(BF16)

            @pl.when(s < last)
            def _():
                hand_on(0, k, ob, xin, xg, above)

            down[k] = value

    def bwd_arrive(k):
        with jax.named_scope("g_wait"):
            remote(gin.at[k], gin.at[k], zs.at[1, k], zr.at[1, k], below).wait_recv()
        with jax.named_scope("g_spread"):
            spread(1, k, gin, gg, near)

    def bwd_hidden(k):
        here = token_rows(k)
        id_col = idc[k]

        def cot_half(c):
            def step(n, carry):
                at = part_cols(c, n, chunk)
                g = gg[k, :, at].astype(F32)
                ct[here, at] = (g * pick(out_tab[:, at], id_col, members)).astype(BF16)
                return carry

            lax.fori_loop(0, half // chunk, step, 0)

        with jax.named_scope("g_gather_wait"):
            gathered(1, k)
            part = gg.at[k, :, core_cols]
            copy = remote(part, part, ds.at[1, k], dr.at[1, k], partner)
            copy.start()
        with jax.named_scope("hidden_own"):
            cot_half(core)
            at = core_cols
            for h, size in pieces:
                hs = slice(h, h + size)
                phid[k, hs, :] = nt_dot(wd[hs, at], ct[here, at])
        with jax.named_scope("g_forward_wait"):
            copy.wait_recv()
        with jax.named_scope("hidden_other"):
            cot_half(other)
            at = cols(other, half)
            for h, size in pieces:
                hs = slice(h, h + size)
                phid[k, hs, :] += nt_dot(wd[hs, at], ct[here, at])

    def bwd_compute(k):
        here = token_rows(k)
        id_col = idc[k]
        with jax.named_scope("grads"):
            scale = inv[k]
            dots = jnp.zeros((total, 1), F32)
            grad_gates = []
            grad_ups = []
            for h, size in pieces:
                hs = slice(h, h + size)
                grad_hidden = phid[k, hs, :].T
                gate = gpre[k, :, hs]
                up = upre[k, :, hs]
                sig = 1.0 / (1.0 + jnp.exp(-gate))
                silu = gate * sig
                mids = grad_hidden * (silu * up)
                for m in range(members):
                    gmid[m : m + 1, hs] += jnp.sum(jnp.where(id_col == m, mids, 0.0), axis=0, keepdims=True)
                grad_product = grad_hidden * pick(mid_tab[:, hs], id_col, members)
                grad_gate = grad_product * up * sig * (1.0 + gate * (1.0 - sig))
                grad_up = grad_product * silu
                dg[here, hs] = (grad_gate * scale).astype(BF16)
                du[here, hs] = (grad_up * scale).astype(BF16)
                grad_gate = grad_gate.astype(BF16)
                grad_up = grad_up.astype(BF16)
                grad_gates.append(grad_gate)
                grad_ups.append(grad_up)
                dots = dots + jnp.sum(
                    grad_gate.astype(F32) * gate + grad_up.astype(F32) * up, axis=-1, keepdims=True
                )
            csend[k] = jnp.broadcast_to(dots, (total, 128)).T[0:8, :]
            ccopy = remote(csend.at[k], cprecv.at[k], cps.at[k], cpr.at[k], partner)
            ccopy.start()
            grad_gates = jnp.concatenate(grad_gates, axis=1)
            grad_ups = jnp.concatenate(grad_ups, axis=1)

        def term(at):
            return jnp.dot(grad_gates, wg[:, at], preferred_element_type=F32) + jnp.dot(
                grad_ups, wu[:, at], preferred_element_type=F32
            )

        def send_dots():
            with jax.named_scope("dots"):
                ccopy.wait_recv()
                cown[k] = csend[k] + cprecv[k]
                for _, device in peers:
                    remote(cown.at[k], crbuf.at[k, q], cs.at[k], cr.at[k], device).start()
                crbuf[k, q] = cown[k]

        reduce_out(1, k, term, send_dots)

    def bwd_finish(k):
        id_col = idc[k]
        g = gin[k].astype(F32)
        grad_scaled = reduced(1, k)
        c15 = crbuf.at[k, pl.ds(0, chips - 1)]
        with jax.named_scope("dots_wait"):
            remote(c15, c15, cs.at[k], cr.at[k], partner).wait_recv()
        with jax.named_scope("bwd_finish"):
            dots = crbuf[k, 0]
            for n in range(1, chips):
                dots = dots + crbuf[k, n]
            mean = dots.T[:, 0:1] * (1.0 / width)
            scale = inv[k]
            normed = xg[k, :, my_cols].astype(F32) * scale
            grad_normed = grad_scaled * pick(gt_tab[:, my_cols], id_col, members)
            ig[k] = (g + scale * (grad_normed - normed * mean)).astype(BF16)

            @pl.when(s > 0)
            def _():
                hand_on(1, k, ig, gin, gg, below)

            outs_here = g * down[k]
            ins_here = grad_scaled * normed
            for m in range(members):
                mask = id_col == m
                acc_out[m : m + 1, :] += jnp.sum(jnp.where(mask, outs_here, 0.0), axis=0, keepdims=True)
                acc_in[m : m + 1, :] += jnp.sum(jnp.where(mask, ins_here, 0.0), axis=0, keepdims=True)

    @pl.when(s == last)
    def _():
        lax.fori_loop(0, micro, lambda k, carry: (bwd_hidden(k), carry)[1], 0)

    behind = jnp.where(s == last, 0, micro + 2)

    large = [
        pltpu.make_async_copy(v, h, hsem.at[n]) for n, (v, h) in enumerate(((sc, sc_h), (ct, ct_h)))
    ]

    def tick(t, carry):
        u = t - behind

        @pl.when(t < micro)
        def _():
            fwd_arrive(t)

        @pl.when(jnp.logical_and(s < last, jnp.logical_and(u >= 0, u < micro)))
        def _():
            bwd_arrive(u)

        @pl.when(jnp.logical_and(t >= 1, t < micro + 1))
        def _():
            fwd_compute(t - 1)

        @pl.when(jnp.logical_and(s < last, jnp.logical_and(u >= 1, u < micro + 1)))
        def _():
            bwd_hidden(u - 1)

        @pl.when(jnp.logical_and(u >= 1, u < micro + 1))
        def _():
            bwd_compute(u - 1)

        @pl.when(u == micro)
        def _():
            for copy in large:
                copy.start()

        @pl.when(jnp.logical_and(t >= 2, t < micro + 2))
        def _():
            fwd_finish(t - 2)

        @pl.when(jnp.logical_and(u >= 2, u < micro + 2))
        def _():
            bwd_finish(u - 2)

        return carry

    lax.fori_loop(0, 2 * (micro + 2), tick, 0)

    with jax.named_scope("end_send"):
        tables = acc_in[...]
        gtl[0:members, :] = tables * gain[:, my_cols]
        gtl[members : 2 * members, :] = acc_out[...]
        gtl[2 * members : 2 * members + 1, :] = jnp.sum(tables * in_tab[:, my_cols], axis=0, keepdims=True)
        gtab[:, my_cols] = gtl[...]
        for _, device in peers:
            remote(gtl, gtab.at[:, my_cols], osem.at[0], osem.at[1], device).start()

        for kind, src in ((0, ob), (1, ig)):
            for k in range(micro):
                rowf[...] = src[k].astype(F32)
                for n in range(chips):
                    for c in range(2):
                        at = (n * 2 + c) * rows
                        outs[n, (c * 2 + kind) * micro + k] = rowf[at : at + rows, :].astype(BF16)
        for to, device in peers:
            remote(outs.at[to], outr.at[:, :, cols(q, bw)], osem.at[2], osem.at[3], device).start()
        outr[:, :, cols(q, bw)] = outs[q]

    with jax.named_scope("end_turn"):
        hid_t[...] = hid[...].T
        dg_t[...] = dg[...].T
        du_t[...] = du[...].T

    with jax.named_scope("end_wait"):
        most = gtab.at[:, pl.ds(0, (chips - 1) * bw)]
        remote(most, most, osem.at[0], osem.at[1], partner).wait_recv()
        table_part = gtab.at[:, core_cols]
        tables_on = remote(table_part, table_part, osem.at[4], osem.at[5], partner)
        tables_on.start()
        most_outs = outs.at[pl.ds(0, chips - 1)]
        remote(most_outs, most_outs, osem.at[2], osem.at[3], partner).wait_recv()
        rows_on = remote(outr.at[pl.ds(other * 2 * micro, 2 * micro)], outp, osem.at[6], osem.at[7], partner)
        rows_on.start()
        out_x[:, :, core_cols] = outr[pl.ds(core * 2 * micro, micro)]
        out_g[:, :, core_cols] = outr[pl.ds((core * 2 + 1) * micro, micro)]

    with jax.named_scope("end_sent"):
        for k in range(micro):
            for ph in range(2):
                remote(r15(ph, k), r15(ph, k), rs.at[ph, k], rr.at[ph, k], partner).wait_send()
                part = psend.at[ph, k, pl.ds(0, chips // 2)]
                for piece in range(2):
                    remote(part, part, ps.at[ph, k, piece], pr.at[ph, k, piece], partner).wait_send()
            remote(csend.at[k], cprecv.at[k], cps.at[k], cpr.at[k], partner).wait_send()
            c15 = crbuf.at[k, pl.ds(0, chips - 1)]
            remote(c15, c15, cs.at[k], cr.at[k], partner).wait_send()
            half_x = xg.at[k, :, core_cols]
            near_x = rbuf.at[0, k, pl.ds(0, len(near))]
            far_x = rbuf.at[0, k, pl.ds(0, len(far) + 1)]
            remote(half_x, half_x, ds.at[1, k], dr.at[1, k], partner).wait_send()

            @pl.when(s == 0)
            def _():
                most_rows = rg.at[pl.ds(0, chips - 1), k]
                remote(most_rows, most_rows, xs.at[k], xr.at[k], partner).wait_send()
                remote(row_part(k, core), row_part(k, core), xds.at[k], xdr.at[k], partner).wait_send()

            @pl.when(s > 0)
            def _():
                remote(near_x, near_x, ags.at[0, k], agr.at[0, k], partner).wait_send()
                remote(half_x, half_x, ds.at[0, k], dr.at[0, k], partner).wait_send()
                remote(far_x, far_x, zs.at[1, k], zr.at[1, k], below).wait_send()

            @pl.when(s < last)
            def _():
                remote(near_x, near_x, ags.at[1, k], agr.at[1, k], partner).wait_send()
                remote(far_x, far_x, zs.at[0, k], zr.at[0, k], above).wait_send()

            @pl.when(s == last)
            def _():
                remote(r15(1, k), r15(1, k), ags.at[1, k], agr.at[1, k], partner).wait_send()

        @pl.when(s == last)
        def _():
            first.wait_send()
            second.wait_send()

        remote(most, most, osem.at[0], osem.at[1], partner).wait_send()
        remote(most_outs, most_outs, osem.at[2], osem.at[3], partner).wait_send()
        for copy in large:
            copy.wait()
    with jax.named_scope("end_out"):
        tables_on.wait()
        g_in[...] = gtab[0:members, :]
        g_out[...] = gtab[members : 2 * members, :]
        g_gain[...] = gtab[2 * members : 2 * members + 1, :]
        rows_on.wait()
        out_x[:, :, cols(other, half)] = outp[0:micro]
        out_g[:, :, cols(other, half)] = outp[micro : 2 * micro]


def weight_grads(hid, dg, du, sc, ct, *refs):
    gate_out, up_out, down_out = refs[len(refs) // 2 - 1 : len(refs) // 2 + 2]
    small = len(refs) // 2 - 1

    def product(left, right, out):
        out[...] = jnp.dot(left[...], right[...], preferred_element_type=F32).astype(BF16)

    product(dg, sc, gate_out)
    product(du, sc, up_out)
    product(hid, ct, down_out)

    @pl.when(pl.program_id(0) == 0)
    def _():
        for src, dst in zip(refs[:small], refs[small + 3 :]):
            dst[...] = src[...]


def on_device(
    tokens, member_ids, cotangent, w_gate, w_up, w_down, in_scale, mid_scale, out_scale, norm_gain
):
    sections = lax.axis_size("section")
    mps = lax.axis_size("mp")
    places = lax.axis_size("dp") // 2
    chips = places * mps
    micro, rows, width = tokens.shape
    total = member_ids.shape[1]
    members = in_scale.shape[1]
    hidden = w_gate.shape[2]
    half = width // 2
    bw = half // chips
    gate_t = w_gate[0].T
    up_t = w_up[0].T
    down_w = w_down[0]
    all_tokens = micro * total
    vmem = pl.BlockSpec(memory_space=pltpu.VMEM)
    hbm = pl.BlockSpec(memory_space=pl.ANY)
    dma = pltpu.SemaphoreType.DMA

    def buf(*shape, dtype=BF16):
        return pltpu.VMEM(shape, dtype)

    dims = (sections, places, mps, micro, rows, members)
    outs = (
        jax.ShapeDtypeStruct((micro, rows, width), BF16),
        jax.ShapeDtypeStruct((micro, rows, width), BF16),
        jax.ShapeDtypeStruct((hidden, all_tokens), BF16),
        jax.ShapeDtypeStruct((hidden, all_tokens), BF16),
        jax.ShapeDtypeStruct((hidden, all_tokens), BF16),
        jax.ShapeDtypeStruct((all_tokens, width), BF16),
        jax.ShapeDtypeStruct((all_tokens, width), BF16),
        jax.ShapeDtypeStruct((members, width), F32),
        jax.ShapeDtypeStruct((members, width), F32),
        jax.ShapeDtypeStruct((1, width), F32),
        jax.ShapeDtypeStruct((members, hidden), F32),
    )
    out_x, out_g, hid, dg, du, sc, ct, g_in, g_out, g_gain, gmid = pl.pallas_call(
        functools.partial(relay_kernel, dims),
        name="relay",
        out_shape=outs,
        in_specs=[vmem, vmem, vmem, hbm, hbm, hbm, vmem, vmem, vmem, vmem],
        out_specs=[vmem] * 5 + [hbm] * 2 + [vmem] * 4,
        scratch_shapes=[
            buf(all_tokens, hidden), buf(all_tokens, hidden), buf(all_tokens, hidden),
            buf(all_tokens, width), buf(all_tokens, width),
            buf(hidden, width), buf(hidden, width), buf(hidden, width),
            buf(2 * chips, micro, rows, width),
            buf(2 * micro, rows, half),
            buf(chips, 2 * micro, rows, bw),
            buf(total, bw, dtype=F32),
            buf(micro, total, bw), buf(micro, total, bw),
            buf(micro, total, width), buf(micro, total, width),
            buf(members, width, dtype=F32),
            buf(micro, total, 1, dtype=jnp.int32),
            buf(micro, total, 1, dtype=F32),
            buf(2, hidden, total, dtype=F32), buf(micro, hidden, total, dtype=F32),
            buf(micro, total, hidden, dtype=F32), buf(micro, total, hidden, dtype=F32),
            buf(2, micro, chips, total, bw), buf(2, micro, chips, total, bw),
            buf(2, micro, chips, total, bw),
            buf(chips, total, bw, dtype=F32),
            buf(2, micro, chips, total, bw),
            buf(micro, 8, total, dtype=F32), buf(micro, 8, total, dtype=F32),
            buf(micro, 8, total, dtype=F32), buf(micro, chips, 8, total, dtype=F32),
            buf(micro, total, bw, dtype=F32),
            buf(micro, total, bw), buf(micro, total, bw),
            buf(members, bw, dtype=F32), buf(members, bw, dtype=F32),
            buf(16, bw, dtype=F32), buf(16, width, dtype=F32),
            buf(chips, 4 * micro, rows, bw),
            buf(4 * micro, rows, half),
            buf(2 * micro, rows, half),
            dma((3,)), dma((2,)), dma((4,)),
            dma((micro,)), dma((micro,)), dma((micro,)), dma((micro,)),
            dma((2, micro)), dma((2, micro)), dma((2, micro)), dma((2, micro)),
            dma((2, micro)), dma((2, micro)), dma((2, micro, 2)), dma((2, micro, 2)),
            dma((2, micro)), dma((2, micro)),
            dma((micro,)), dma((micro,)), dma((micro,)), dma((micro,)),
            dma((8,)),
        ],
        compiler_params=pltpu.CompilerParams(
            collective_id=0, has_side_effects=True, vmem_limit_bytes=56 * 1024 * 1024
        ),
    )(
        tokens, cotangent, member_ids, gate_t, up_t, down_w,
        in_scale[0], norm_gain, out_scale[0], mid_scale[0],
    )

    step = min(512, width)
    whole = pl.BlockSpec((hidden, all_tokens), lambda n: (0, 0))
    tall = pl.BlockSpec((all_tokens, step), lambda n: (0, n))
    wide = pl.BlockSpec((hidden, step), lambda n: (0, n))
    small = (out_x, out_g, g_in, g_out, g_gain, gmid)
    passed = [pl.BlockSpec(a.shape, lambda n, d=a.ndim: (0,) * d) for a in small]
    grad_gate, grad_up, grad_down, *small = pl.pallas_call(
        weight_grads,
        name="weight_grads",
        grid=(width // step,),
        out_shape=[jax.ShapeDtypeStruct((hidden, width), BF16)] * 3
        + [jax.ShapeDtypeStruct(a.shape, a.dtype) for a in small],
        in_specs=[whole, whole, whole, tall, tall] + passed,
        out_specs=[wide] * 3 + passed,
    )(hid, dg, du, sc, ct, *small)
    out_x, out_g, g_in, g_out, g_gain, gmid = small

    return (
        out_x[None],
        out_g[None],
        grad_gate.T[None],
        grad_up.T[None],
        grad_down[None],
        g_in[None],
        gmid[None],
        g_out[None],
        g_gain,
    )


def solution(mesh):
    in_specs = (
        P(None, ("dp", "mp"), None),
        P(),
        P(None, ("dp", "mp"), None),
        P("section", None, ("dp", "mp")),
        P("section", None, ("dp", "mp")),
        P("section", ("dp", "mp"), None),
        P("section", None, None),
        P("section", None, ("dp", "mp")),
        P("section", None, None),
        P("section", None),
    )
    out_specs = (
        P("section", None, ("dp", "mp"), None),
        P("section", None, ("dp", "mp"), None),
        P("section", None, ("dp", "mp")),
        P("section", None, ("dp", "mp")),
        P("section", ("dp", "mp"), None),
        P("section", None, None),
        P("section", None, ("dp", "mp")),
        P("section", None, None),
        P("section", None),
    )
    return jax.shard_map(
        on_device, mesh=mesh, in_specs=in_specs, out_specs=out_specs, check_vma=False
    )
```

```python
import functools

import jax
import jax.numpy as jnp
from jax import lax
from jax.experimental import pallas as pl
from jax.experimental.pallas import tpu as pltpu
from jax.sharding import PartitionSpec as P

EPS = 1e-05
F32 = jnp.float32
BF16 = jnp.bfloat16


def nt_dot(left, right):
    return lax.dot_general(left, right, (((1,), (1,)), ((), ())), preferred_element_type=F32)


def pick(table, ids, members):
    rows = ids.shape[0]
    value = jnp.broadcast_to(table[members - 1 : members], (rows, table.shape[1]))
    for m in range(members - 1):
        value = jnp.where(ids == m, table[m : m + 1], value)
    return value


def relay_kernel(
    dims,
    tok_h, cot_h, ids_h, in_h, gain_h, out_h, mid_h, wg_h, wu_h, wd_h,
    out_x, out_g, g_gate, g_up, g_down, g_in, g_out, g_gain, gmid,
    tok, cot, ids, in_tab, gain, out_tab, mid_tab, in_rows, out_rows,
    hid, dg, du, sc, ct, turned,
    wg, wu, wd, rg, t1, initr, rowf, xin, gin, xg, gg, gt_tab, idc, inv, pacc, phid, gpre, upre,
    psend, precv, pown, pf, rbuf, csend, cprecv, cown, crbuf, down, ob, ig,
    acc_in, acc_out, gtl, gtab, outs, outr, outp,
    insem, wsem, isem, xs, xr, xds, xdr, zs, zr, ags, agr, ds, dr, ps, pr, rs, rr, cps, cpr, cs, cr, osem,
):
    sections, places, mps, micro, rows, members = dims
    chips = places * mps
    across = places // 2
    width = in_tab.shape[1]
    hidden = mid_tab.shape[1]
    half = width // 2
    bw = half // chips
    total = rows * 2 * chips
    s = lax.axis_index("section")
    dp = lax.axis_index("dp")
    mp = lax.axis_index("mp")
    core = lax.rem(dp, 2)
    other = 1 - core
    place = dp // 2
    along_x = lax.rem(place, across)
    y_low = place // across
    along_y = mp * 2 + y_low
    q = place * mps + mp
    block = core * chips + q
    last = sections - 1
    partner = {"dp": place * 2 + other, "mp": mp}
    up_s = jnp.minimum(s + 1, last)
    down_s = jnp.maximum(s - 1, 0)
    above = {"section": up_s}
    below = {"section": down_s}

    def hops(d):
        return min(d[0], across - d[0]) + min(d[1], 2 * mps - d[1])

    offsets = [(dx, dy) for dx in range(across) for dy in range(2 * mps) if dx or dy]
    offsets.sort(key=lambda d: -hops(d))
    reach = hops(offsets[0]) // 2

    def chip(dx, dy):
        x = lax.rem(along_x + dx, across)
        y = lax.rem(along_y + dy, 2 * mps)
        at = lax.rem(y, 2) * across + x
        return at * mps + y // 2, {"dp": at * 2 + core, "mp": y // 2}

    peers = [chip(*d) for d in offsets]
    far = [p for p, d in zip(peers, offsets) if hops(d) > reach]
    near = [p for p, d in zip(peers, offsets) if hops(d) <= reach]
    groups = [
        [p for p, d in zip(peers, offsets) if d[1] % 2 == 0],
        [p for p, d in zip(peers, offsets) if d[1] % 2 == 1],
    ]

    def remote(src, dst, send, recv, device):
        return pltpu.make_async_remote_copy(
            src_ref=src, dst_ref=dst, send_sem=send, recv_sem=recv,
            device_id=device, device_id_type=pl.DeviceIdType.MESH,
        )

    def cols(index, size):
        return pl.ds(pl.multiple_of(index * size, size), size)

    inputs = [
        pltpu.make_async_copy(h, v, insem.at[i])
        for i, (h, v) in enumerate(
            (
                (tok_h, tok), (cot_h, cot), (ids_h, ids), (in_h, in_tab),
                (gain_h, gain), (out_h, out_tab), (mid_h, mid_tab),
            )
        )
    ]
    for copy in inputs:
        copy.start()
    weights = [
        pltpu.make_async_copy(h, v, wsem.at[i])
        for i, (h, v) in enumerate(((wg_h, wg), (wu_h, wu), (wd_h, wd)))
    ]
    for copy in weights:
        copy.start()

    init_scope = jax.named_scope("init_local")
    init_scope.__enter__()
    barrier = pltpu.get_barrier_semaphore()
    for _, device in peers:
        pl.semaphore_signal(barrier, inc=1, device_id=device, device_id_type=pl.DeviceIdType.MESH)
    pl.semaphore_signal(barrier, inc=1, device_id=partner, device_id_type=pl.DeviceIdType.MESH)

    @pl.when(s < last)
    def _():
        for device in [above] + [{**d, **above} for _, d in far]:
            pl.semaphore_signal(barrier, inc=1, device_id=device, device_id_type=pl.DeviceIdType.MESH)

    @pl.when(s > 0)
    def _():
        for device in [below] + [{**d, **below} for _, d in far]:
            pl.semaphore_signal(barrier, inc=1, device_id=device, device_id_type=pl.DeviceIdType.MESH)

    for copy in inputs:
        copy.wait()
    init_scope.__exit__(None, None, None)
    links = (s < last).astype(jnp.int32) + (s > 0).astype(jnp.int32)
    with jax.named_scope("init_barrier"):
        pl.semaphore_wait(barrier, chips + (1 + len(far)) * links)

    my_cols = cols(block, bw)
    core_cols = cols(core, half)
    r15 = lambda ph, k: rbuf.at[ph, k, pl.ds(0, chips - 1)]

    def spread(ph, k, src, dst, targets):
        for _, device in targets:
            remote(src.at[k], dst.at[k, :, my_cols], ags.at[ph, k], agr.at[ph, k], device).start()
        dst[k, :, my_cols] = src[k]

    def hand_on(ph, k, src, dst, gathered, section):
        remote(src.at[k], dst.at[k], zs.at[ph, k], zr.at[ph, k], section).start()
        for _, device in far:
            remote(
                src.at[k], gathered.at[k, :, my_cols], zs.at[ph, k], agr.at[ph, k], {**device, **section}
            ).start()

    row_part = lambda k, c: rg.at[pl.ds(c * chips, chips), k]

    @pl.when(s == 0)
    def _():
        for k in range(micro):
            for _, device in peers:
                remote(tok.at[k], rg.at[block, k], xs.at[k], xr.at[k], device).start()
            rg[block, k] = tok[k]

    def forward_rows(k):
        most_rows = rg.at[pl.ds(0, chips - 1), k]
        remote(most_rows, most_rows, xs.at[k], xr.at[k], partner).wait_recv()
        remote(row_part(k, core), row_part(k, core), xds.at[k], xdr.at[k], partner).start()

    def place_rows(k):
        remote(row_part(k, other), row_part(k, other), xds.at[k], xdr.at[k], partner).wait_recv()
        for c in range(2):
            for n in range(chips):
                at = (n * 2 + c) * rows
                xg[k, at : at + rows, :] = rg[c * chips + n, k]

    chunk = min(512, half)
    gt_tab[...] = in_tab[...] * gain[...]
    acc_in[...] = jnp.zeros_like(acc_in)
    acc_out[...] = jnp.zeros_like(acc_out)
    gmid[...] = jnp.zeros_like(gmid)
    gtl[...] = jnp.zeros_like(gtl)
    i = lax.broadcasted_iota(jnp.int32, (total, total), 0)
    j = lax.broadcasted_iota(jnp.int32, (total, total), 1)
    i_mp = (i // (2 * rows)) % mps
    i_core = (i // rows) % 2
    source = (((i // (2 * rows * mps)) * 2 + i_core) * mps + i_mp) * rows + i % rows
    for k in range(micro):
        picked = jnp.where(source == j, jnp.broadcast_to(ids[k : k + 1, :], (total, total)), 0)
        idc[k] = jnp.sum(picked.astype(F32), axis=1, keepdims=True).astype(jnp.int32)
    for k in range(micro):
        for at in range(0, width, chunk):
            here = slice(at, at + chunk)
            in_rows[k, :, here] = pick(gt_tab[:, here], idc[k], members)
            out_rows[k, :, here] = pick(out_tab[:, here], idc[k], members)

    mine = pl.ds(core * micro, micro)
    first = remote(cot.at[:, :, cols(other, half)], t1.at[mine], isem.at[0], isem.at[1], partner)
    others = initr.at[pl.ds(0, chips - 1)]
    second = remote(others, others, isem.at[2], isem.at[3], partner)

    @pl.when(s == last)
    def _():
        first.start()
        t1[mine] = cot[:, :, cols(core, half)]
        first.wait_recv()
        for to, device in peers:
            remote(t1.at[:, :, cols(to, bw)], initr.at[q], isem.at[2], isem.at[3], device).start()
        initr[q] = t1[:, :, cols(q, bw)]
        second.wait_recv()
        for k in range(micro):
            for n in range(chips):
                for c in range(2):
                    at = (n * 2 + c) * rows
                    rowf[at : at + rows, :] = initr[n, c * micro + k].astype(F32)
            gin[k] = rowf[...].astype(BF16)
            spread(1, k, gin, gg, peers)

    with jax.named_scope("init_weights"):
        for copy in weights:
            copy.wait()

    pieces = [(at, min(256, hidden - at)) for at in range(0, hidden, 256)]

    def part_cols(c, n, size):
        return pl.ds(pl.multiple_of(c * half + n * size, size), size)

    def gathered(ph, k):
        remote(r15(ph, k), r15(ph, k), ags.at[ph, k], agr.at[ph, k], partner).wait_recv()

    def reduce_out(ph, k, term, between=None):
        step = min(512, half // 2)
        each = step // bw
        halves = half // 2 // step
        copies = []
        for piece in range(2):
            low = y_low if piece == 0 else 1 - y_low
            with jax.named_scope("down_other"):
                for n in range(halves):
                    at = other * half + low * (half // 2) + n * step
                    value = term(pl.ds(pl.multiple_of(at, step), step))
                    for e in range(each):
                        to = low * (chips // 2) + n * each + e
                        psend[ph, k, to] = value[:, e * bw : (e + 1) * bw].astype(BF16)
            at = pl.ds(low * (chips // 2), chips // 2)
            copy = remote(
                psend.at[ph, k, at], precv.at[ph, k, at], ps.at[ph, k, piece], pr.at[ph, k, piece], partner
            )
            copy.start()
            copies.append(copy)
        with jax.named_scope("down_own"):
            for n in range(half // step):
                value = term(pl.ds(pl.multiple_of(core * half + n * step, step), step))
                for e in range(each):
                    pf[n * each + e] = value[:, e * bw : (e + 1) * bw]
        if between is not None:
            between()
        for piece in range(2):
            low = y_low if piece == 0 else 1 - y_low
            with jax.named_scope("partner_wait"):
                copies[piece].wait_recv()
            with jax.named_scope("combine"):
                for n in range(chips // 2):
                    at = low * (chips // 2) + n
                    pown[ph, k, at] = (pf[at] + precv[ph, k, at].astype(F32)).astype(BF16)
                for to, device in groups[piece]:
                    remote(pown.at[ph, k, to], rbuf.at[ph, k, q], rs.at[ph, k], rr.at[ph, k], device).start()
        rbuf[ph, k, q] = pown[ph, k, q]

    def reduced(ph, k):
        with jax.named_scope("reduce_wait"):
            remote(r15(ph, k), r15(ph, k), rs.at[ph, k], rr.at[ph, k], partner).wait_recv()
        value = rbuf[ph, k, 0].astype(F32)
        for n in range(1, chips):
            value = value + rbuf[ph, k, n].astype(F32)
        return value

    def token_rows(k):
        return pl.ds(pl.multiple_of(k * total, total), total)

    def member_sums(acc, id_col, value):
        for m in range(members):
            acc[m : m + 1, :] += jnp.sum(jnp.where(id_col == m, value, 0.0), axis=0, keepdims=True)

    def fwd_arrive(k):
        with jax.named_scope("x_wait"):
            @pl.when(s > 0)
            def _():
                remote(xin.at[k], xin.at[k], zs.at[0, k], zr.at[0, k], above).wait_recv()
                spread(0, k, xin, xg, near)

            @pl.when(jnp.logical_and(s == 0, k == 0))
            def _():
                forward_rows(k)

    def fwd_compute(k):
        here = token_rows(k)
        id_col = idc[k]

        def scaled_half(c, squares):
            def step(n, carry):
                at = part_cols(c, n, chunk)
                x = xg[k, :, at].astype(F32)
                sc[here, at] = (x * in_rows[k, :, at]).astype(BF16)
                x2 = x * x
                for e in range(chunk // 128):
                    carry = carry + x2[:, e * 128 : (e + 1) * 128]
                return carry

            return lax.fori_loop(0, half // chunk, step, squares)

        part = xg.at[k, :, core_cols]
        copy = remote(part, part, ds.at[0, k], dr.at[0, k], partner)
        with jax.named_scope("gather_wait"):
            @pl.when(s > 0)
            def _():
                gathered(0, k)
                copy.start()

            @pl.when(s == 0)
            def _():
                place_rows(k)

        with jax.named_scope("gateup_own"):
            squares = scaled_half(core, jnp.zeros((total, 128), F32))
            at = core_cols
            for h, size in pieces:
                hs = slice(h, h + size)
                pacc[0, hs, :] = nt_dot(wg[hs, at], sc[here, at])
                pacc[1, hs, :] = nt_dot(wu[hs, at], sc[here, at])
        with jax.named_scope("forward_wait"):
            @pl.when(s > 0)
            def _():
                copy.wait_recv()

            @pl.when(jnp.logical_and(s == 0, k < micro - 1))
            def _():
                forward_rows(jnp.minimum(k + 1, micro - 1))

        with jax.named_scope("gateup_other"):
            squares = scaled_half(other, squares)
            scale = lax.rsqrt(jnp.sum(squares, axis=-1, keepdims=True) * (1.0 / width) + EPS)
            inv[k] = scale
            at = cols(other, half)
            for h, size in pieces:
                hs = slice(h, h + size)
                gate = (pacc[0, hs, :] + nt_dot(wg[hs, at], sc[here, at])).T * scale
                up = (pacc[1, hs, :] + nt_dot(wu[hs, at], sc[here, at])).T * scale
                gpre[k, :, hs] = gate
                upre[k, :, hs] = up
                product = gate / (1.0 + jnp.exp(-gate)) * up
                hid[here, hs] = (product * pick(mid_tab[:, hs], id_col, members)).astype(BF16)

    def fwd_down(k):
        h = hid[token_rows(k), :]
        reduce_out(0, k, lambda at: jnp.dot(h, wd[:, at], preferred_element_type=F32))

    def fwd_finish(k):
        value = reduced(0, k)
        with jax.named_scope("fwd_finish"):
            x = xg[k, :, my_cols].astype(F32)
            ob[k] = (x + value * out_rows[k, :, my_cols]).astype(BF16)

            @pl.when(s < last)
            def _():
                hand_on(0, k, ob, xin, xg, above)

            down[k] = value

    def bwd_arrive(k):
        with jax.named_scope("g_wait"):
            remote(gin.at[k], gin.at[k], zs.at[1, k], zr.at[1, k], below).wait_recv()
        with jax.named_scope("g_spread"):
            spread(1, k, gin, gg, near)

    def bwd_hidden(k):
        here = token_rows(k)

        def cot_half(c):
            def step(n, carry):
                at = part_cols(c, n, chunk)
                g = gg[k, :, at].astype(F32)
                ct[here, at] = (g * out_rows[k, :, at]).astype(BF16)
                return carry

            lax.fori_loop(0, half // chunk, step, 0)

        with jax.named_scope("g_gather_wait"):
            gathered(1, k)
            part = gg.at[k, :, core_cols]
            copy = remote(part, part, ds.at[1, k], dr.at[1, k], partner)
            copy.start()
        with jax.named_scope("hidden_own"):
            cot_half(core)
            at = core_cols
            for h, size in pieces:
                hs = slice(h, h + size)
                phid[k, hs, :] = nt_dot(wd[hs, at], ct[here, at])
        with jax.named_scope("g_forward_wait"):
            copy.wait_recv()
        with jax.named_scope("hidden_other"):
            cot_half(other)
            at = cols(other, half)
            for h, size in pieces:
                hs = slice(h, h + size)
                phid[k, hs, :] += nt_dot(wd[hs, at], ct[here, at])

    def bwd_compute(k):
        here = token_rows(k)
        id_col = idc[k]
        with jax.named_scope("grads"):
            scale = inv[k]
            dots = jnp.zeros((total, 1), F32)
            grad_gates = []
            grad_ups = []
            for h, size in pieces:
                hs = slice(h, h + size)
                grad_hidden = phid[k, hs, :].T
                gate = gpre[k, :, hs]
                up = upre[k, :, hs]
                sig = 1.0 / (1.0 + jnp.exp(-gate))
                silu = gate * sig
                mids = grad_hidden * (silu * up)
                for m in range(members):
                    gmid[m : m + 1, hs] += jnp.sum(jnp.where(id_col == m, mids, 0.0), axis=0, keepdims=True)
                grad_product = grad_hidden * pick(mid_tab[:, hs], id_col, members)
                grad_gate = grad_product * up * sig * (1.0 + gate * (1.0 - sig))
                grad_up = grad_product * silu
                dg[here, hs] = (grad_gate * scale).astype(BF16)
                du[here, hs] = (grad_up * scale).astype(BF16)
                grad_gate = grad_gate.astype(BF16)
                grad_up = grad_up.astype(BF16)
                grad_gates.append(grad_gate)
                grad_ups.append(grad_up)
                dots = dots + jnp.sum(
                    grad_gate.astype(F32) * gate + grad_up.astype(F32) * up, axis=-1, keepdims=True
                )
            csend[k] = jnp.broadcast_to(dots, (total, 128)).T[0:8, :]
            ccopy = remote(csend.at[k], cprecv.at[k], cps.at[k], cpr.at[k], partner)
            ccopy.start()
            grad_gates = jnp.concatenate(grad_gates, axis=1)
            grad_ups = jnp.concatenate(grad_ups, axis=1)

        def term(at):
            return jnp.dot(grad_gates, wg[:, at], preferred_element_type=F32) + jnp.dot(
                grad_ups, wu[:, at], preferred_element_type=F32
            )

        def send_dots():
            with jax.named_scope("dots"):
                ccopy.wait_recv()
                cown[k] = csend[k] + cprecv[k]
                for _, device in peers:
                    remote(cown.at[k], crbuf.at[k, q], cs.at[k], cr.at[k], device).start()
                crbuf[k, q] = cown[k]

        reduce_out(1, k, term, send_dots)

    def bwd_finish(k):
        id_col = idc[k]
        g = gin[k].astype(F32)
        grad_scaled = reduced(1, k)
        c15 = crbuf.at[k, pl.ds(0, chips - 1)]
        with jax.named_scope("dots_wait"):
            remote(c15, c15, cs.at[k], cr.at[k], partner).wait_recv()
        with jax.named_scope("bwd_finish"):
            dots = crbuf[k, 0]
            for n in range(1, chips):
                dots = dots + crbuf[k, n]
            mean = dots.T[:, 0:1] * (1.0 / width)
            scale = inv[k]
            normed = xg[k, :, my_cols].astype(F32) * scale
            grad_normed = grad_scaled * in_rows[k, :, my_cols]
            ig[k] = (g + scale * (grad_normed - normed * mean)).astype(BF16)

            @pl.when(s > 0)
            def _():
                hand_on(1, k, ig, gin, gg, below)

            member_sums(acc_in, id_col, grad_scaled * normed)

    def out_scale_grad(k):
        member_sums(acc_out, idc[k], gin[k].astype(F32) * down[k])

    @pl.when(s == last)
    def _():
        lax.fori_loop(0, micro, lambda k, carry: (bwd_hidden(k), carry)[1], 0)

    behind = jnp.where(s == last, 0, micro + 2)
    down_behind = jnp.where(s == last, micro + 2, 1)

    def weight_grads():
        wide = min(1024, width)
        with jax.named_scope("weight_grads"):
            for left, right, out in ((dg, sc, g_gate), (du, sc, g_up), (hid, ct, g_down)):
                turned[...] = left[...].T

                def step(n, carry):
                    at = cols(n, wide)
                    out[:, at] = jnp.dot(turned[...], right[:, at], preferred_element_type=F32).astype(BF16)
                    return carry

                lax.fori_loop(0, width // wide, step, 0)

    def tick(t, carry):
        u = t - behind
        d = t - down_behind

        @pl.when(t < micro)
        def _():
            fwd_arrive(t)

        @pl.when(jnp.logical_and(s < last, jnp.logical_and(u >= 0, u < micro)))
        def _():
            bwd_arrive(u)

        @pl.when(jnp.logical_and(t >= 1, t < micro + 1))
        def _():
            fwd_compute(t - 1)

        @pl.when(jnp.logical_and(d >= 0, d < micro))
        def _():
            fwd_down(d)

        @pl.when(jnp.logical_and(s < last, jnp.logical_and(u >= 1, u < micro + 1)))
        def _():
            bwd_hidden(u - 1)

        @pl.when(jnp.logical_and(u >= 1, u < micro + 1))
        def _():
            bwd_compute(u - 1)

        @pl.when(jnp.logical_and(s == 0, u == micro + 1))
        def _():
            weight_grads()

        @pl.when(jnp.logical_and(d >= 1, d < micro + 1))
        def _():
            fwd_finish(d - 1)

        @pl.when(jnp.logical_and(s == last, jnp.logical_and(d >= 1, d < micro + 1)))
        def _():
            out_scale_grad(d - 1)

        @pl.when(jnp.logical_and(u >= 2, u < micro + 2))
        def _():
            bwd_finish(u - 2)

        @pl.when(jnp.logical_and(s < last, jnp.logical_and(u >= 2, u < micro + 2)))
        def _():
            out_scale_grad(u - 2)

        @pl.when(jnp.logical_and(s > 0, u == micro + 1))
        def _():
            weight_grads()

        return carry

    lax.fori_loop(0, 2 * (micro + 2), tick, 0)

    with jax.named_scope("end_send"):
        tables = acc_in[...]
        gtl[0:members, :] = tables * gain[:, my_cols]
        gtl[members : 2 * members, :] = acc_out[...]
        gtl[2 * members : 2 * members + 1, :] = jnp.sum(tables * in_tab[:, my_cols], axis=0, keepdims=True)
        gtab[:, my_cols] = gtl[...]
        for _, device in peers:
            remote(gtl, gtab.at[:, my_cols], osem.at[0], osem.at[1], device).start()

        for kind, src in ((0, ob), (1, ig)):
            for k in range(micro):
                rowf[...] = src[k].astype(F32)
                for n in range(chips):
                    for c in range(2):
                        at = (n * 2 + c) * rows
                        outs[n, (c * 2 + kind) * micro + k] = rowf[at : at + rows, :].astype(BF16)
        for to, device in peers:
            remote(outs.at[to], outr.at[:, :, cols(q, bw)], osem.at[2], osem.at[3], device).start()
        outr[:, :, cols(q, bw)] = outs[q]

    with jax.named_scope("end_wait"):
        most = gtab.at[:, pl.ds(0, (chips - 1) * bw)]
        remote(most, most, osem.at[0], osem.at[1], partner).wait_recv()
        table_part = gtab.at[:, core_cols]
        tables_on = remote(table_part, table_part, osem.at[4], osem.at[5], partner)
        tables_on.start()
        most_outs = outs.at[pl.ds(0, chips - 1)]
        remote(most_outs, most_outs, osem.at[2], osem.at[3], partner).wait_recv()
        rows_on = remote(outr.at[pl.ds(other * 2 * micro, 2 * micro)], outp, osem.at[6], osem.at[7], partner)
        rows_on.start()
        out_x[:, :, core_cols] = outr[pl.ds(core * 2 * micro, micro)]
        out_g[:, :, core_cols] = outr[pl.ds((core * 2 + 1) * micro, micro)]

    with jax.named_scope("end_sent"):
        for k in range(micro):
            for ph in range(2):
                remote(r15(ph, k), r15(ph, k), rs.at[ph, k], rr.at[ph, k], partner).wait_send()
                part = psend.at[ph, k, pl.ds(0, chips // 2)]
                for piece in range(2):
                    remote(part, part, ps.at[ph, k, piece], pr.at[ph, k, piece], partner).wait_send()
            remote(csend.at[k], cprecv.at[k], cps.at[k], cpr.at[k], partner).wait_send()
            c15 = crbuf.at[k, pl.ds(0, chips - 1)]
            remote(c15, c15, cs.at[k], cr.at[k], partner).wait_send()
            half_x = xg.at[k, :, core_cols]
            near_x = rbuf.at[0, k, pl.ds(0, len(near))]
            far_x = rbuf.at[0, k, pl.ds(0, len(far) + 1)]
            remote(half_x, half_x, ds.at[1, k], dr.at[1, k], partner).wait_send()

            @pl.when(s == 0)
            def _():
                most_rows = rg.at[pl.ds(0, chips - 1), k]
                remote(most_rows, most_rows, xs.at[k], xr.at[k], partner).wait_send()
                remote(row_part(k, core), row_part(k, core), xds.at[k], xdr.at[k], partner).wait_send()

            @pl.when(s > 0)
            def _():
                remote(near_x, near_x, ags.at[0, k], agr.at[0, k], partner).wait_send()
                remote(half_x, half_x, ds.at[0, k], dr.at[0, k], partner).wait_send()
                remote(far_x, far_x, zs.at[1, k], zr.at[1, k], below).wait_send()

            @pl.when(s < last)
            def _():
                remote(near_x, near_x, ags.at[1, k], agr.at[1, k], partner).wait_send()
                remote(far_x, far_x, zs.at[0, k], zr.at[0, k], above).wait_send()

            @pl.when(s == last)
            def _():
                remote(r15(1, k), r15(1, k), ags.at[1, k], agr.at[1, k], partner).wait_send()

        @pl.when(s == last)
        def _():
            first.wait_send()
            second.wait_send()

        remote(most, most, osem.at[0], osem.at[1], partner).wait_send()
        remote(most_outs, most_outs, osem.at[2], osem.at[3], partner).wait_send()
    with jax.named_scope("end_out"):
        tables_on.wait()
        g_in[...] = gtab[0:members, :]
        g_out[...] = gtab[members : 2 * members, :]
        g_gain[...] = gtab[2 * members : 2 * members + 1, :]
        rows_on.wait()
        out_x[:, :, cols(other, half)] = outp[0:micro]
        out_g[:, :, cols(other, half)] = outp[micro : 2 * micro]


def deliver(count, *refs):
    sems = refs[-1]
    copies = [
        pltpu.make_async_copy(src, dst, sems.at[n])
        for n, (src, dst) in enumerate(zip(refs[:count], refs[count : 2 * count]))
    ]
    for copy in copies:
        copy.start()
    for copy in copies:
        copy.wait()


def on_device(
    tokens, member_ids, cotangent, w_gate, w_up, w_down, in_scale, mid_scale, out_scale, norm_gain
):
    sections = lax.axis_size("section")
    mps = lax.axis_size("mp")
    places = lax.axis_size("dp") // 2
    chips = places * mps
    micro, rows, width = tokens.shape
    total = member_ids.shape[1]
    members = in_scale.shape[1]
    hidden = w_gate.shape[2]
    half = width // 2
    bw = half // chips
    gate_t = w_gate[0].T
    up_t = w_up[0].T
    down_w = w_down[0]
    all_tokens = micro * total
    vmem = pl.BlockSpec(memory_space=pltpu.VMEM)
    hbm = pl.BlockSpec(memory_space=pl.ANY)
    dma = pltpu.SemaphoreType.DMA

    def buf(*shape, dtype=BF16):
        return pltpu.VMEM(shape, dtype)

    dims = (sections, places, mps, micro, rows, members)
    outs = (
        pltpu.VMEM((micro, rows, width), BF16),
        pltpu.VMEM((micro, rows, width), BF16),
        pltpu.VMEM((hidden, width), BF16),
        pltpu.VMEM((hidden, width), BF16),
        pltpu.VMEM((hidden, width), BF16),
        pltpu.VMEM((members, width), F32),
        pltpu.VMEM((members, width), F32),
        pltpu.VMEM((1, width), F32),
        pltpu.VMEM((members, hidden), F32),
    )
    results = pl.pallas_call(
        functools.partial(relay_kernel, dims),
        name="relay",
        out_shape=outs,
        in_specs=[pl.BlockSpec(memory_space=pltpu.HBM)] * 10,
        out_specs=[vmem] * len(outs),
        scratch_shapes=[
            buf(micro, rows, width), buf(micro, rows, width), buf(micro, total, dtype=jnp.int32),
            buf(members, width, dtype=F32), buf(1, width, dtype=F32),
            buf(members, width, dtype=F32), buf(members, hidden, dtype=F32),
            buf(micro, total, width, dtype=F32), buf(micro, total, width, dtype=F32),
            buf(all_tokens, hidden), buf(all_tokens, hidden), buf(all_tokens, hidden),
            buf(all_tokens, width), buf(all_tokens, width), buf(hidden, all_tokens),
            buf(hidden, width), buf(hidden, width), buf(hidden, width),
            buf(2 * chips, micro, rows, width),
            buf(2 * micro, rows, half),
            buf(chips, 2 * micro, rows, bw),
            buf(total, bw, dtype=F32),
            buf(micro, total, bw), buf(micro, total, bw),
            buf(micro, total, width), buf(micro, total, width),
            buf(members, width, dtype=F32),
            buf(micro, total, 1, dtype=jnp.int32),
            buf(micro, total, 1, dtype=F32),
            buf(2, hidden, total, dtype=F32), buf(micro, hidden, total, dtype=F32),
            buf(micro, total, hidden, dtype=F32), buf(micro, total, hidden, dtype=F32),
            buf(2, micro, chips, total, bw), buf(2, micro, chips, total, bw),
            buf(2, micro, chips, total, bw),
            buf(chips, total, bw, dtype=F32),
            buf(2, micro, chips, total, bw),
            buf(micro, 8, total, dtype=F32), buf(micro, 8, total, dtype=F32),
            buf(micro, 8, total, dtype=F32), buf(micro, chips, 8, total, dtype=F32),
            buf(micro, total, bw, dtype=F32),
            buf(micro, total, bw), buf(micro, total, bw),
            buf(members, bw, dtype=F32), buf(members, bw, dtype=F32),
            buf(16, bw, dtype=F32), buf(16, width, dtype=F32),
            buf(chips, 4 * micro, rows, bw),
            buf(4 * micro, rows, half),
            buf(2 * micro, rows, half),
            dma((7,)), dma((3,)), dma((4,)),
            dma((micro,)), dma((micro,)), dma((micro,)), dma((micro,)),
            dma((2, micro)), dma((2, micro)), dma((2, micro)), dma((2, micro)),
            dma((2, micro)), dma((2, micro)), dma((2, micro, 2)), dma((2, micro, 2)),
            dma((2, micro)), dma((2, micro)),
            dma((micro,)), dma((micro,)), dma((micro,)), dma((micro,)),
            dma((8,)),
        ],
        compiler_params=pltpu.CompilerParams(
            collective_id=0, has_side_effects=True, vmem_limit_bytes=46 * 1024 * 1024
        ),
    )(
        tokens, cotangent, member_ids, in_scale[0], norm_gain, out_scale[0], mid_scale[0],
        gate_t, up_t, down_w,
    )

    out_x, out_g, grad_gate, grad_up, grad_down, g_in, g_out, g_gain, gmid = pl.pallas_call(
        functools.partial(deliver, len(outs)),
        name="deliver",
        out_shape=[jax.ShapeDtypeStruct(o.shape, o.dtype) for o in outs],
        in_specs=[vmem] * len(outs),
        out_specs=[hbm] * len(outs),
        scratch_shapes=[dma((len(outs),))],
        compiler_params=pltpu.CompilerParams(vmem_limit_bytes=1024 * 1024),
    )(*[pltpu.with_memory_space_constraint(r, pltpu.VMEM) for r in results])

    return (
        out_x[None],
        out_g[None],
        grad_gate.T[None],
        grad_up.T[None],
        grad_down[None],
        g_in[None],
        gmid[None],
        g_out[None],
        g_gain,
    )


def solution(mesh):
    in_specs = (
        P(None, ("dp", "mp"), None),
        P(),
        P(None, ("dp", "mp"), None),
        P("section", None, ("dp", "mp")),
        P("section", None, ("dp", "mp")),
        P("section", ("dp", "mp"), None),
        P("section", None, None),
        P("section", None, ("dp", "mp")),
        P("section", None, None),
        P("section", None),
    )
    out_specs = (
        P("section", None, ("dp", "mp"), None),
        P("section", None, ("dp", "mp"), None),
        P("section", None, ("dp", "mp")),
        P("section", None, ("dp", "mp")),
        P("section", ("dp", "mp"), None),
        P("section", None, None),
        P("section", None, ("dp", "mp")),
        P("section", None, None),
        P("section", None),
    )
    return jax.shard_map(
        on_device, mesh=mesh, in_specs=in_specs, out_specs=out_specs, check_vma=False
    )
```

```python
import functools

import jax
import jax.numpy as jnp
from jax import lax
from jax.experimental import pallas as pl
from jax.experimental.pallas import tpu as pltpu
from jax.sharding import PartitionSpec as P

EPS = 1e-05
F32 = jnp.float32
BF16 = jnp.bfloat16


def nt_dot(left, right):
    return lax.dot_general(left, right, (((1,), (1,)), ((), ())), preferred_element_type=F32)


def pick(table, ids, members):
    rows = ids.shape[0]
    value = jnp.broadcast_to(table[members - 1 : members], (rows, table.shape[1]))
    for m in range(members - 1):
        value = jnp.where(ids == m, table[m : m + 1], value)
    return value


def relay_kernel(
    dims,
    tok_h, cot_h, ids_h, in_h, gain_h, out_h, mid_h, wg_h, wu_h, wd_h,
    out_x, out_g, g_gate, g_up, g_down, g_in, g_out, g_gain, gmid,
    tok, cot, ids, in_tab, gain, out_tab, mid_tab, in_rows, out_rows,
    hid, dg, du, sc, ct, turned, ggate, gup, gmids,
    wgu, wd, rg, t1, initr, rowf, xin, gin, xg, gg, gt_tab, idc, inv, pacc, phid, gpre, upre,
    psend, precv, pown, pf, rbuf, csend, cprecv, cown, crbuf, down, ob, ig,
    acc_in, acc_out, gtl, gtab, outs, outr, outp,
    insem, wsem, isem, xs, xr, xds, xdr, zs, zr, ags, agr, ds, dr, ps, pr, rs, rr, cps, cpr, cs, cr, osem,
):
    sections, places, mps, micro, rows, members = dims
    chips = places * mps
    across = places // 2
    width = in_tab.shape[1]
    hidden = mid_tab.shape[1]
    half = width // 2
    bw = half // chips
    total = rows * 2 * chips
    s = lax.axis_index("section")
    dp = lax.axis_index("dp")
    mp = lax.axis_index("mp")
    core = lax.rem(dp, 2)
    other = 1 - core
    place = dp // 2
    along_x = lax.rem(place, across)
    y_low = place // across
    along_y = mp * 2 + y_low
    q = place * mps + mp
    block = core * chips + q
    last = sections - 1
    partner = {"dp": place * 2 + other, "mp": mp}
    up_s = jnp.minimum(s + 1, last)
    down_s = jnp.maximum(s - 1, 0)
    above = {"section": up_s}
    below = {"section": down_s}

    def hops(d):
        return min(d[0], across - d[0]) + min(d[1], 2 * mps - d[1])

    offsets = [(dx, dy) for dx in range(across) for dy in range(2 * mps) if dx or dy]
    def ups(d):
        return (d[0] if d[0] * 2 <= across else 0) + (d[1] if d[1] <= mps else 0)

    offsets.sort(key=lambda d: (-ups(d), -hops(d)))
    reach = max(map(hops, offsets)) // 2

    def chip(dx, dy):
        x = lax.rem(along_x + dx, across)
        y = lax.rem(along_y + dy, 2 * mps)
        at = lax.rem(y, 2) * across + x
        return at * mps + y // 2, {"dp": at * 2 + core, "mp": y // 2}

    peers = [chip(*d) for d in offsets]
    far = [p for p, d in zip(peers, offsets) if hops(d) > reach]
    near = [p for p, d in zip(peers, offsets) if hops(d) <= reach]
    groups = [
        [p for p, d in zip(peers, offsets) if d[1] % 2 == 0],
        [p for p, d in zip(peers, offsets) if d[1] % 2 == 1],
    ]

    def remote(src, dst, send, recv, device):
        return pltpu.make_async_remote_copy(
            src_ref=src, dst_ref=dst, send_sem=send, recv_sem=recv,
            device_id=device, device_id_type=pl.DeviceIdType.MESH,
        )

    def cols(index, size):
        return pl.ds(pl.multiple_of(index * size, size), size)

    wg = wgu.at[0:hidden]
    wu = wgu.at[hidden : 2 * hidden]
    inputs = [
        pltpu.make_async_copy(h, v, insem.at[i])
        for i, (h, v) in enumerate(
            (
                (tok_h, tok), (cot_h, cot), (ids_h, ids), (in_h, in_tab),
                (gain_h, gain), (out_h, out_tab), (mid_h, mid_tab),
            )
        )
    ]
    for copy in inputs:
        copy.start()
    weights = [
        pltpu.make_async_copy(h, v, wsem.at[i])
        for i, (h, v) in enumerate(((wg_h, wg), (wu_h, wu), (wd_h, wd)))
    ]
    for copy in weights:
        copy.start()

    barrier = pltpu.get_barrier_semaphore()
    for _, device in peers:
        pl.semaphore_signal(barrier, inc=1, device_id=device, device_id_type=pl.DeviceIdType.MESH)
    pl.semaphore_signal(barrier, inc=1, device_id=partner, device_id_type=pl.DeviceIdType.MESH)

    @pl.when(s < last)
    def _():
        for device in [above] + [{**d, **above} for _, d in far]:
            pl.semaphore_signal(barrier, inc=1, device_id=device, device_id_type=pl.DeviceIdType.MESH)

    @pl.when(s > 0)
    def _():
        for device in [below] + [{**d, **below} for _, d in far]:
            pl.semaphore_signal(barrier, inc=1, device_id=device, device_id_type=pl.DeviceIdType.MESH)

    with jax.named_scope("init_local"):
        for copy in inputs:
            copy.wait()
    links = (s < last).astype(jnp.int32) + (s > 0).astype(jnp.int32)
    with jax.named_scope("init_barrier"):
        pl.semaphore_wait(barrier, chips + (1 + len(far)) * links)

    my_cols = cols(block, bw)
    core_cols = cols(core, half)
    r15 = lambda ph, k: rbuf.at[ph, k, pl.ds(0, chips - 1)]

    def spread(ph, k, src, dst, targets):
        for _, device in targets:
            remote(src.at[k], dst.at[k, :, my_cols], ags.at[ph, k], agr.at[ph, k], device).start()
        dst[k, :, my_cols] = src[k]

    def hand_on(ph, k, src, dst, gathered, section):
        remote(src.at[k], dst.at[k], zs.at[ph, k], zr.at[ph, k], section).start()
        for _, device in far:
            remote(
                src.at[k], gathered.at[k, :, my_cols], zs.at[ph, k], agr.at[ph, k], {**device, **section}
            ).start()

    row_part = lambda k, c: rg.at[pl.ds(c * chips, chips), k]

    @pl.when(s == 0)
    def _():
        for k in range(micro):
            for _, device in peers:
                remote(tok.at[k], rg.at[block, k], xs.at[k], xr.at[k], device).start()
            rg[block, k] = tok[k]

    def forward_rows(k):
        most_rows = rg.at[pl.ds(0, chips - 1), k]
        remote(most_rows, most_rows, xs.at[k], xr.at[k], partner).wait_recv()
        remote(row_part(k, core), row_part(k, core), xds.at[k], xdr.at[k], partner).start()

    def place_rows(k):
        remote(row_part(k, other), row_part(k, other), xds.at[k], xdr.at[k], partner).wait_recv()
        for c in range(2):
            for n in range(chips):
                at = (n * 2 + c) * rows
                xg[k, at : at + rows, :] = rg[c * chips + n, k]

    chunk = min(512, half)
    gt_tab[...] = in_tab[...] * gain[...]
    acc_in[...] = jnp.zeros_like(acc_in)
    acc_out[...] = jnp.zeros_like(acc_out)
    gmid[...] = jnp.zeros_like(gmid)
    gtl[...] = jnp.zeros_like(gtl)
    i = lax.broadcasted_iota(jnp.int32, (total, total), 0)
    j = lax.broadcasted_iota(jnp.int32, (total, total), 1)
    i_mp = (i // (2 * rows)) % mps
    i_core = (i // rows) % 2
    source = (((i // (2 * rows * mps)) * 2 + i_core) * mps + i_mp) * rows + i % rows
    for k in range(micro):
        picked = jnp.where(source == j, jnp.broadcast_to(ids[k : k + 1, :], (total, total)), 0)
        idc[k] = jnp.sum(picked.astype(F32), axis=1, keepdims=True).astype(jnp.int32)
    for k in range(micro):
        for at in range(0, width, chunk):
            here = slice(at, at + chunk)
            in_rows[k, :, here] = pick(gt_tab[:, here], idc[k], members)
            out_rows[k, :, here] = pick(out_tab[:, here], idc[k], members)

    mine = pl.ds(core * micro, micro)
    first = remote(cot.at[:, :, cols(other, half)], t1.at[mine], isem.at[0], isem.at[1], partner)
    others = initr.at[pl.ds(0, chips - 1)]
    second = remote(others, others, isem.at[2], isem.at[3], partner)

    @pl.when(s == last)
    def _():
        first.start()
        t1[mine] = cot[:, :, cols(core, half)]
        first.wait_recv()
        for to, device in peers:
            remote(t1.at[:, :, cols(to, bw)], initr.at[q], isem.at[2], isem.at[3], device).start()
        initr[q] = t1[:, :, cols(q, bw)]
        second.wait_recv()
        for k in range(micro):
            for n in range(chips):
                for c in range(2):
                    at = (n * 2 + c) * rows
                    rowf[at : at + rows, :] = initr[n, c * micro + k].astype(F32)
            gin[k] = rowf[...].astype(BF16)
            spread(1, k, gin, gg, peers)

    with jax.named_scope("init_weights"):
        for copy in weights:
            copy.wait()

    pieces = [(at, min(256, hidden - at)) for at in range(0, hidden, 256)]

    def part_cols(c, n, size):
        return pl.ds(pl.multiple_of(c * half + n * size, size), size)

    def gathered(ph, k):
        remote(r15(ph, k), r15(ph, k), ags.at[ph, k], agr.at[ph, k], partner).wait_recv()

    def reduce_out(ph, k, term, between=None):
        step = min(512, half // 2)
        each = step // bw
        halves = half // 2 // step
        copies = []
        for piece in range(2):
            low = y_low if piece == 0 else 1 - y_low
            with jax.named_scope("down_other"):
                for n in range(halves):
                    at = other * half + low * (half // 2) + n * step
                    value = term(pl.ds(pl.multiple_of(at, step), step))
                    for e in range(each):
                        to = low * (chips // 2) + n * each + e
                        psend[ph, k, to] = value[:, e * bw : (e + 1) * bw].astype(BF16)
            at = pl.ds(low * (chips // 2), chips // 2)
            copy = remote(
                psend.at[ph, k, at], precv.at[ph, k, at], ps.at[ph, k, piece], pr.at[ph, k, piece], partner
            )
            copy.start()
            copies.append(copy)
        with jax.named_scope("down_own"):
            for n in range(half // step):
                value = term(pl.ds(pl.multiple_of(core * half + n * step, step), step))
                for e in range(each):
                    pf[n * each + e] = value[:, e * bw : (e + 1) * bw]
        if between is not None:
            between()
        for piece in range(2):
            low = y_low if piece == 0 else 1 - y_low
            with jax.named_scope("partner_wait"):
                copies[piece].wait_recv()
            with jax.named_scope("combine"):
                for n in range(chips // 2):
                    at = low * (chips // 2) + n
                    pown[ph, k, at] = (pf[at] + precv[ph, k, at].astype(F32)).astype(BF16)
                for to, device in groups[piece]:
                    remote(pown.at[ph, k, to], rbuf.at[ph, k, q], rs.at[ph, k], rr.at[ph, k], device).start()
        rbuf[ph, k, q] = pown[ph, k, q]

    def reduced(ph, k):
        with jax.named_scope("reduce_wait"):
            remote(r15(ph, k), r15(ph, k), rs.at[ph, k], rr.at[ph, k], partner).wait_recv()
        value = rbuf[ph, k, 0].astype(F32)
        for n in range(1, chips):
            value = value + rbuf[ph, k, n].astype(F32)
        return value

    def token_rows(k):
        return pl.ds(pl.multiple_of(k * total, total), total)

    def member_sums(acc, id_col, value):
        for m in range(members):
            acc[m : m + 1, :] += jnp.sum(jnp.where(id_col == m, value, 0.0), axis=0, keepdims=True)

    def fwd_arrive(k):
        with jax.named_scope("x_wait"):
            @pl.when(s > 0)
            def _():
                remote(xin.at[k], xin.at[k], zs.at[0, k], zr.at[0, k], above).wait_recv()
                spread(0, k, xin, xg, near)

            @pl.when(jnp.logical_and(s == 0, k == 0))
            def _():
                forward_rows(k)

    def fwd_compute(k):
        here = token_rows(k)
        id_col = idc[k]

        def scaled_half(c, squares):
            def step(n, carry):
                at = part_cols(c, n, chunk)
                x = xg[k, :, at].astype(F32)
                sc[here, at] = (x * in_rows[k, :, at]).astype(BF16)
                x2 = x * x
                for e in range(chunk // 128):
                    carry = carry + x2[:, e * 128 : (e + 1) * 128]
                return carry

            return lax.fori_loop(0, half // chunk, step, squares)

        part = xg.at[k, :, core_cols]
        copy = remote(part, part, ds.at[0, k], dr.at[0, k], partner)
        with jax.named_scope("gather_wait"):
            @pl.when(s > 0)
            def _():
                gathered(0, k)
                copy.start()

            @pl.when(s == 0)
            def _():
                place_rows(k)

        with jax.named_scope("gateup_own"):
            squares = scaled_half(core, jnp.zeros((total, 128), F32))
            at = core_cols
            for h, size in pieces:
                hs = slice(h, h + size)
                pacc[0, hs, :] = nt_dot(wg[hs, at], sc[here, at])
                pacc[1, hs, :] = nt_dot(wu[hs, at], sc[here, at])
        with jax.named_scope("forward_wait"):
            @pl.when(s > 0)
            def _():
                copy.wait_recv()
        with jax.named_scope("gateup_other"):
            squares = scaled_half(other, squares)
            scale = lax.rsqrt(jnp.sum(squares, axis=-1, keepdims=True) * (1.0 / width) + EPS)
            inv[k] = scale
            at = cols(other, half)
            for h, size in pieces:
                hs = slice(h, h + size)
                gate = (pacc[0, hs, :] + nt_dot(wg[hs, at], sc[here, at])).T * scale
                up = (pacc[1, hs, :] + nt_dot(wu[hs, at], sc[here, at])).T * scale
                gpre[k, :, hs] = gate
                upre[k, :, hs] = up
                product = gate / (1.0 + jnp.exp(-gate)) * up
                hid[here, hs] = (product * pick(mid_tab[:, hs], id_col, members)).astype(BF16)

    def fwd_down(k):
        @pl.when(jnp.logical_and(s == 0, k < micro - 1))
        def _():
            forward_rows(jnp.minimum(k + 1, micro - 1))

        h = hid[token_rows(k), :]
        reduce_out(0, k, lambda at: jnp.dot(h, wd[:, at], preferred_element_type=F32))

    def fwd_finish(k):
        value = reduced(0, k)
        with jax.named_scope("fwd_finish"):
            x = xg[k, :, my_cols].astype(F32)
            ob[k] = (x + value * out_rows[k, :, my_cols]).astype(BF16)

            @pl.when(s < last)
            def _():
                hand_on(0, k, ob, xin, xg, above)

            down[k] = value

    def bwd_arrive(k):
        with jax.named_scope("g_wait"):
            remote(gin.at[k], gin.at[k], zs.at[1, k], zr.at[1, k], below).wait_recv()
        with jax.named_scope("g_spread"):
            spread(1, k, gin, gg, near)

    def bwd_hidden(k):
        here = token_rows(k)

        def cot_half(c):
            def step(n, carry):
                at = part_cols(c, n, chunk)
                g = gg[k, :, at].astype(F32)
                ct[here, at] = (g * out_rows[k, :, at]).astype(BF16)
                return carry

            lax.fori_loop(0, half // chunk, step, 0)

        with jax.named_scope("g_gather_wait"):
            gathered(1, k)
            part = gg.at[k, :, core_cols]
            copy = remote(part, part, ds.at[1, k], dr.at[1, k], partner)
            copy.start()
        with jax.named_scope("hidden_own"):
            cot_half(core)
            at = core_cols
            for h, size in pieces:
                hs = slice(h, h + size)
                phid[k, hs, :] = nt_dot(wd[hs, at], ct[here, at])
        with jax.named_scope("g_forward_wait"):
            copy.wait_recv()
        with jax.named_scope("hidden_other"):
            cot_half(other)
            at = cols(other, half)
            for h, size in pieces:
                hs = slice(h, h + size)
                phid[k, hs, :] += nt_dot(wd[hs, at], ct[here, at])

    def bwd_compute(k):
        here = token_rows(k)
        id_col = idc[k]
        with jax.named_scope("grads"):
            scale = inv[k]
            dots = jnp.zeros((total, 1), F32)
            grad_pre = []
            grad_ups = []
            for h, size in pieces:
                hs = slice(h, h + size)
                grad_hidden = phid[k, hs, :].T
                gate = gpre[k, :, hs]
                up = upre[k, :, hs]
                sig = 1.0 / (1.0 + jnp.exp(-gate))
                silu = gate * sig
                grad_product = grad_hidden * pick(mid_tab[:, hs], id_col, members)
                grad_gate = grad_product * up * sig * (1.0 + gate * (1.0 - sig))
                grad_up = grad_product * silu
                ggate[:, hs] = grad_gate
                gup[:, hs] = grad_up
                gmids[:, hs] = grad_hidden * (silu * up)
                grad_gate = grad_gate.astype(BF16)
                grad_up = grad_up.astype(BF16)
                grad_pre.append(grad_gate)
                grad_ups.append(grad_up)
                dots = dots + jnp.sum(
                    grad_gate.astype(F32) * gate + grad_up.astype(F32) * up, axis=-1, keepdims=True
                )
            csend[k] = jnp.broadcast_to(dots, (total, 128)).T[0:1, :]
            ccopy = remote(csend.at[k], cprecv.at[k], cps.at[k], cpr.at[k], partner)
            ccopy.start()
            pre = jnp.concatenate(grad_pre + grad_ups, axis=1)

        def term(at):
            return jnp.dot(pre, wgu[:, at], preferred_element_type=F32)

        def send_dots():
            with jax.named_scope("dots"):
                ccopy.wait_recv()
                cown[k] = csend[k] + cprecv[k]
                for _, device in peers:
                    remote(cown.at[k], crbuf.at[k, q], cs.at[k], cr.at[k], device).start()
                crbuf[k, q] = cown[k]
            with jax.named_scope("keep"):
                dg[here, :] = (ggate[...] * scale).astype(BF16)
                du[here, :] = (gup[...] * scale).astype(BF16)
                member_sums(gmid, id_col, gmids[...])

        reduce_out(1, k, term, send_dots)

    def bwd_finish(k):
        id_col = idc[k]
        c15 = crbuf.at[k, pl.ds(0, chips - 1)]
        with jax.named_scope("dots_wait"):
            remote(c15, c15, cs.at[k], cr.at[k], partner).wait_recv()
            dots = crbuf[k, 0]
            for n in range(1, chips):
                dots = dots + crbuf[k, n]
            mean = jnp.broadcast_to(dots, (8, total)).T[:, 0:1] * (1.0 / width)
            scale = inv[k]
            g = gin[k].astype(F32)
            normed = xg[k, :, my_cols].astype(F32) * scale
            kept = g - scale * mean * normed
        grad_scaled = reduced(1, k)
        with jax.named_scope("bwd_finish"):
            grad_normed = grad_scaled * in_rows[k, :, my_cols]
            ig[k] = (kept + scale * grad_normed).astype(BF16)

            @pl.when(s > 0)
            def _():
                hand_on(1, k, ig, gin, gg, below)

            member_sums(acc_in, id_col, grad_scaled * normed)

    def out_scale_grad(k):
        member_sums(acc_out, idc[k], gin[k].astype(F32) * down[k])

    @pl.when(s == last)
    def _():
        lax.fori_loop(0, micro, lambda k, carry: (bwd_hidden(k), carry)[1], 0)

    behind = jnp.where(s == last, 0, micro + 2)
    down_behind = jnp.where(s == last, micro + 2, 1)

    def weight_grads():
        wide = min(1024, width)
        with jax.named_scope("weight_grads"):
            for left, right, out in ((dg, sc, g_gate), (du, sc, g_up), (hid, ct, g_down)):
                turned[...] = left[...].T

                def step(n, carry):
                    at = cols(n, wide)
                    out[:, at] = jnp.dot(turned[...], right[:, at], preferred_element_type=F32).astype(BF16)
                    return carry

                lax.fori_loop(0, width // wide, step, 0)

    def send_rows(kind, src):
        for k in range(micro):
            rowf[...] = src[k].astype(F32)
            for n in range(chips):
                for c in range(2):
                    at = (n * 2 + c) * rows
                    outs[kind, n, c * micro + k] = rowf[at : at + rows, :].astype(BF16)
        for to, device in peers:
            remote(
                outs.at[kind, to], outr.at[kind, :, :, cols(q, bw)],
                osem.at[kind], osem.at[2 + kind], device,
            ).start()
        outr[kind, :, :, cols(q, bw)] = outs[kind, q]

    def tick(t, carry):
        u = t - behind
        d = t - down_behind

        @pl.when(t < micro)
        def _():
            fwd_arrive(t)

        @pl.when(jnp.logical_and(s < last, jnp.logical_and(u >= 0, u < micro)))
        def _():
            bwd_arrive(u)

        @pl.when(jnp.logical_and(t >= 1, t < micro + 1))
        def _():
            fwd_compute(t - 1)

        @pl.when(jnp.logical_and(d >= 0, d < micro))
        def _():
            fwd_down(d)

        @pl.when(jnp.logical_and(s < last, jnp.logical_and(u >= 1, u < micro + 1)))
        def _():
            bwd_hidden(u - 1)

        @pl.when(jnp.logical_and(u >= 1, u < micro + 1))
        def _():
            bwd_compute(u - 1)

        @pl.when(jnp.logical_and(s == 0, u == micro + 1))
        def _():
            weight_grads()

        @pl.when(jnp.logical_and(d >= 1, d < micro + 1))
        def _():
            fwd_finish(d - 1)

        @pl.when(jnp.logical_and(s == last, jnp.logical_and(d >= 1, d < micro + 1)))
        def _():
            out_scale_grad(d - 1)

        @pl.when(d == micro)
        def _():
            send_rows(0, ob)

        @pl.when(jnp.logical_and(u >= 2, u < micro + 2))
        def _():
            bwd_finish(u - 2)

        @pl.when(jnp.logical_and(s < last, jnp.logical_and(u >= 2, u < micro + 2)))
        def _():
            out_scale_grad(u - 2)

        @pl.when(jnp.logical_and(s > 0, u == micro + 1))
        def _():
            weight_grads()

        return carry

    lax.fori_loop(0, 2 * (micro + 2), tick, 0)

    with jax.named_scope("end_send"):
        tables = acc_in[...]
        gtl[0:members, :] = tables * gain[:, my_cols]
        gtl[members : 2 * members, :] = acc_out[...]
        gtl[2 * members : 2 * members + 1, :] = jnp.sum(tables * in_tab[:, my_cols], axis=0, keepdims=True)
        gtab[:, my_cols] = gtl[...]
        for _, device in peers:
            remote(gtl, gtab.at[:, my_cols], osem.at[4], osem.at[5], device).start()
        send_rows(1, ig)

    with jax.named_scope("end_wait"):
        most = gtab.at[:, pl.ds(0, (chips - 1) * bw)]
        most_outs = [outs.at[kind, pl.ds(0, chips - 1)] for kind in range(2)]
        rows_on = [
            remote(
                outr.at[kind, pl.ds(other * micro, micro)], outp.at[kind],
                osem.at[6 + kind], osem.at[8 + kind], partner,
            )
            for kind in range(2)
        ]
        remote(most_outs[0], most_outs[0], osem.at[0], osem.at[2], partner).wait_recv()
        rows_on[0].start()
        remote(most, most, osem.at[4], osem.at[5], partner).wait_recv()
        table_part = gtab.at[:, core_cols]
        tables_on = remote(table_part, table_part, osem.at[10], osem.at[11], partner)
        tables_on.start()
        remote(most_outs[1], most_outs[1], osem.at[1], osem.at[3], partner).wait_recv()
        rows_on[1].start()
        out_x[:, :, core_cols] = outr[0, pl.ds(core * micro, micro)]
        out_g[:, :, core_cols] = outr[1, pl.ds(core * micro, micro)]

    with jax.named_scope("end_sent"):
        for k in range(micro):
            for ph in range(2):
                remote(r15(ph, k), r15(ph, k), rs.at[ph, k], rr.at[ph, k], partner).wait_send()
                part = psend.at[ph, k, pl.ds(0, chips // 2)]
                for piece in range(2):
                    remote(part, part, ps.at[ph, k, piece], pr.at[ph, k, piece], partner).wait_send()
            remote(csend.at[k], cprecv.at[k], cps.at[k], cpr.at[k], partner).wait_send()
            c15 = crbuf.at[k, pl.ds(0, chips - 1)]
            remote(c15, c15, cs.at[k], cr.at[k], partner).wait_send()
            half_x = xg.at[k, :, core_cols]
            near_x = rbuf.at[0, k, pl.ds(0, len(near))]
            far_x = rbuf.at[0, k, pl.ds(0, len(far) + 1)]
            remote(half_x, half_x, ds.at[1, k], dr.at[1, k], partner).wait_send()

            @pl.when(s == 0)
            def _():
                most_rows = rg.at[pl.ds(0, chips - 1), k]
                remote(most_rows, most_rows, xs.at[k], xr.at[k], partner).wait_send()
                remote(row_part(k, core), row_part(k, core), xds.at[k], xdr.at[k], partner).wait_send()

            @pl.when(s > 0)
            def _():
                remote(near_x, near_x, ags.at[0, k], agr.at[0, k], partner).wait_send()
                remote(half_x, half_x, ds.at[0, k], dr.at[0, k], partner).wait_send()
                remote(far_x, far_x, zs.at[1, k], zr.at[1, k], below).wait_send()

            @pl.when(s < last)
            def _():
                remote(near_x, near_x, ags.at[1, k], agr.at[1, k], partner).wait_send()
                remote(far_x, far_x, zs.at[0, k], zr.at[0, k], above).wait_send()

            @pl.when(s == last)
            def _():
                remote(r15(1, k), r15(1, k), ags.at[1, k], agr.at[1, k], partner).wait_send()

        @pl.when(s == last)
        def _():
            first.wait_send()
            second.wait_send()

        remote(most, most, osem.at[4], osem.at[5], partner).wait_send()
        for kind in range(2):
            remote(most_outs[kind], most_outs[kind], osem.at[kind], osem.at[2 + kind], partner).wait_send()
    with jax.named_scope("end_out"):
        tables_on.wait()
        g_in[...] = gtab[0:members, :]
        g_out[...] = gtab[members : 2 * members, :]
        g_gain[...] = gtab[2 * members : 2 * members + 1, :]
        rows_on[0].wait()
        out_x[:, :, cols(other, half)] = outp[0]
        rows_on[1].wait()
        out_g[:, :, cols(other, half)] = outp[1]


def deliver(count, *refs):
    sems = refs[-1]
    copies = [
        pltpu.make_async_copy(src, dst, sems.at[n])
        for n, (src, dst) in enumerate(zip(refs[:count], refs[count : 2 * count]))
    ]
    for copy in copies:
        copy.start()
    for copy in copies:
        copy.wait()


def on_device(
    tokens, member_ids, cotangent, w_gate, w_up, w_down, in_scale, mid_scale, out_scale, norm_gain
):
    sections = lax.axis_size("section")
    mps = lax.axis_size("mp")
    places = lax.axis_size("dp") // 2
    chips = places * mps
    micro, rows, width = tokens.shape
    total = member_ids.shape[1]
    members = in_scale.shape[1]
    hidden = w_gate.shape[2]
    half = width // 2
    bw = half // chips
    gate_t = w_gate[0].T
    up_t = w_up[0].T
    down_w = w_down[0]
    all_tokens = micro * total
    vmem = pl.BlockSpec(memory_space=pltpu.VMEM)
    hbm = pl.BlockSpec(memory_space=pl.ANY)
    dma = pltpu.SemaphoreType.DMA

    def buf(*shape, dtype=BF16):
        return pltpu.VMEM(shape, dtype)

    dims = (sections, places, mps, micro, rows, members)
    outs = (
        pltpu.VMEM((micro, rows, width), BF16),
        pltpu.VMEM((micro, rows, width), BF16),
        pltpu.VMEM((hidden, width), BF16),
        pltpu.VMEM((hidden, width), BF16),
        pltpu.VMEM((hidden, width), BF16),
        pltpu.VMEM((members, width), F32),
        pltpu.VMEM((members, width), F32),
        pltpu.VMEM((1, width), F32),
        pltpu.VMEM((members, hidden), F32),
    )
    results = pl.pallas_call(
        functools.partial(relay_kernel, dims),
        name="relay",
        out_shape=outs,
        in_specs=[pl.BlockSpec(memory_space=pltpu.HBM)] * 10,
        out_specs=[vmem] * len(outs),
        scratch_shapes=[
            buf(micro, rows, width), buf(micro, rows, width), buf(micro, total, dtype=jnp.int32),
            buf(members, width, dtype=F32), buf(1, width, dtype=F32),
            buf(members, width, dtype=F32), buf(members, hidden, dtype=F32),
            buf(micro, total, width, dtype=F32), buf(micro, total, width, dtype=F32),
            buf(all_tokens, hidden), buf(all_tokens, hidden), buf(all_tokens, hidden),
            buf(all_tokens, width), buf(all_tokens, width), buf(hidden, all_tokens),
            buf(total, hidden, dtype=F32), buf(total, hidden, dtype=F32), buf(total, hidden, dtype=F32),
            buf(2 * hidden, width), buf(hidden, width),
            buf(2 * chips, micro, rows, width),
            buf(2 * micro, rows, half),
            buf(chips, 2 * micro, rows, bw),
            buf(total, bw, dtype=F32),
            buf(micro, total, bw), buf(micro, total, bw),
            buf(micro, total, width), buf(micro, total, width),
            buf(members, width, dtype=F32),
            buf(micro, total, 1, dtype=jnp.int32),
            buf(micro, total, 1, dtype=F32),
            buf(2, hidden, total, dtype=F32), buf(micro, hidden, total, dtype=F32),
            buf(micro, total, hidden, dtype=F32), buf(micro, total, hidden, dtype=F32),
            buf(2, micro, chips, total, bw), buf(2, micro, chips, total, bw),
            buf(2, micro, chips, total, bw),
            buf(chips, total, bw, dtype=F32),
            buf(2, micro, chips, total, bw),
            buf(micro, 1, total, dtype=F32), buf(micro, 1, total, dtype=F32),
            buf(micro, 1, total, dtype=F32), buf(micro, chips, 1, total, dtype=F32),
            buf(micro, total, bw, dtype=F32),
            buf(micro, total, bw), buf(micro, total, bw),
            buf(members, bw, dtype=F32), buf(members, bw, dtype=F32),
            buf(16, bw, dtype=F32), buf(16, width, dtype=F32),
            buf(2, chips, 2 * micro, rows, bw),
            buf(2, 2 * micro, rows, half),
            buf(2, micro, rows, half),
            dma((7,)), dma((3,)), dma((4,)),
            dma((micro,)), dma((micro,)), dma((micro,)), dma((micro,)),
            dma((2, micro)), dma((2, micro)), dma((2, micro)), dma((2, micro)),
            dma((2, micro)), dma((2, micro)), dma((2, micro, 2)), dma((2, micro, 2)),
            dma((2, micro)), dma((2, micro)),
            dma((micro,)), dma((micro,)), dma((micro,)), dma((micro,)),
            dma((12,)),
        ],
        compiler_params=pltpu.CompilerParams(
            collective_id=0, has_side_effects=True, vmem_limit_bytes=46 * 1024 * 1024
        ),
    )(
        tokens, cotangent, member_ids, in_scale[0], norm_gain, out_scale[0], mid_scale[0],
        gate_t, up_t, down_w,
    )

    out_x, out_g, grad_gate, grad_up, grad_down, g_in, g_out, g_gain, gmid = pl.pallas_call(
        functools.partial(deliver, len(outs)),
        name="deliver",
        out_shape=[jax.ShapeDtypeStruct(o.shape, o.dtype) for o in outs],
        in_specs=[vmem] * len(outs),
        out_specs=[hbm] * len(outs),
        scratch_shapes=[dma((len(outs),))],
        compiler_params=pltpu.CompilerParams(vmem_limit_bytes=1024 * 1024),
    )(*[pltpu.with_memory_space_constraint(r, pltpu.VMEM) for r in results])

    return (
        out_x[None],
        out_g[None],
        grad_gate.T[None],
        grad_up.T[None],
        grad_down[None],
        g_in[None],
        gmid[None],
        g_out[None],
        g_gain,
    )


def solution(mesh):
    in_specs = (
        P(None, ("dp", "mp"), None),
        P(),
        P(None, ("dp", "mp"), None),
        P("section", None, ("dp", "mp")),
        P("section", None, ("dp", "mp")),
        P("section", ("dp", "mp"), None),
        P("section", None, None),
        P("section", None, ("dp", "mp")),
        P("section", None, None),
        P("section", None),
    )
    out_specs = (
        P("section", None, ("dp", "mp"), None),
        P("section", None, ("dp", "mp"), None),
        P("section", None, ("dp", "mp")),
        P("section", None, ("dp", "mp")),
        P("section", ("dp", "mp"), None),
        P("section", None, None),
        P("section", None, ("dp", "mp")),
        P("section", None, None),
        P("section", None),
    )
    return jax.shard_map(
        on_device, mesh=mesh, in_specs=in_specs, out_specs=out_specs, check_vma=False
    )
```

```python
import functools

import jax
import jax.numpy as jnp
from jax import lax
from jax.experimental import pallas as pl
from jax.experimental.pallas import tpu as pltpu
from jax.sharding import PartitionSpec as P

EPS = 1e-05
F32 = jnp.float32
BF16 = jnp.bfloat16


def nt_dot(left, right):
    return lax.dot_general(left, right, (((1,), (1,)), ((), ())), preferred_element_type=F32)


def pick(table, ids, members):
    rows = ids.shape[0]
    value = jnp.broadcast_to(table[members - 1 : members], (rows, table.shape[1]))
    for m in range(members - 1):
        value = jnp.where(ids == m, table[m : m + 1], value)
    return value


def relay_kernel(
    dims,
    tok_h, cot_h, ids_h, in_h, gain_h, out_h, mid_h, wg_h, wu_h, wd_h,
    out_x, out_g, g_gate, g_up, g_down, g_in, g_out, g_gain, gmid,
    tok, cot, ids, in_tab, gain, out_tab, mid_tab, in_rows, out_rows,
    hid, dg, du, sc, ct, turned, ggate, gup, gmids,
    wgu, wd, rg, t1, initr, rowf, xin, gin, xg, gg, gt_tab, idc, inv, pacc, phid, gpre, upre,
    psend, precv, pown, pf, rbuf, csend, cprecv, cown, crbuf, down, ob, ig,
    acc_in, acc_out, gtl, gtab, outs, outr, outp,
    insem, wsem, isem, xs, xr, xds, xdr, zs, zr, ags, agr, ds, dr, ps, pr, rs, rr, cps, cpr, cs, cr, osem,
):
    sections, places, mps, micro, rows, members = dims
    chips = places * mps
    across = places // 2
    width = in_tab.shape[1]
    hidden = mid_tab.shape[1]
    half = width // 2
    bw = half // chips
    total = rows * 2 * chips
    s = lax.axis_index("section")
    dp = lax.axis_index("dp")
    mp = lax.axis_index("mp")
    core = lax.rem(dp, 2)
    other = 1 - core
    place = dp // 2
    along_x = lax.rem(place, across)
    y_low = place // across
    along_y = mp * 2 + y_low
    q = place * mps + mp
    block = core * chips + q
    last = sections - 1
    partner = {"dp": place * 2 + other, "mp": mp}
    up_s = jnp.minimum(s + 1, last)
    down_s = jnp.maximum(s - 1, 0)
    above = {"section": up_s}
    below = {"section": down_s}

    def hops(d):
        return min(d[0], across - d[0]) + min(d[1], 2 * mps - d[1])

    offsets = [(dx, dy) for dx in range(across) for dy in range(2 * mps) if dx or dy]
    def ups(d):
        return (d[0] if d[0] * 2 <= across else 0) + (d[1] if d[1] <= mps else 0)

    def downs(d):
        x, y = (across - d[0]) % across, (2 * mps - d[1]) % (2 * mps)
        return (x if x * 2 <= across else 0) + (y if y <= mps else 0)

    offsets.sort(key=lambda d: (-downs(d), -hops(d)))
    reach = max(map(hops, offsets)) // 2

    def chip(dx, dy):
        x = lax.rem(along_x + dx, across)
        y = lax.rem(along_y + dy, 2 * mps)
        at = lax.rem(y, 2) * across + x
        return at * mps + y // 2, {"dp": at * 2 + core, "mp": y // 2}

    peers = [chip(*d) for d in offsets]
    far = [p for p, d in zip(peers, offsets) if hops(d) > reach]
    near = [p for p, d in zip(peers, offsets) if hops(d) <= reach]
    groups = [
        [p for p, d in zip(peers, offsets) if d[1] % 2 == 0],
        [p for p, d in zip(peers, offsets) if d[1] % 2 == 1],
    ]

    def remote(src, dst, send, recv, device):
        return pltpu.make_async_remote_copy(
            src_ref=src, dst_ref=dst, send_sem=send, recv_sem=recv,
            device_id=device, device_id_type=pl.DeviceIdType.MESH,
        )

    def cols(index, size):
        return pl.ds(pl.multiple_of(index * size, size), size)

    wg = wgu.at[0:hidden]
    wu = wgu.at[hidden : 2 * hidden]
    inputs = [
        pltpu.make_async_copy(h, v, insem.at[i])
        for i, (h, v) in enumerate(
            (
                (tok_h, tok), (cot_h, cot), (ids_h, ids), (in_h, in_tab),
                (gain_h, gain), (out_h, out_tab), (mid_h, mid_tab),
            )
        )
    ]
    for copy in inputs:
        copy.start()
    weights = [
        pltpu.make_async_copy(h, v, wsem.at[i])
        for i, (h, v) in enumerate(((wg_h, wg), (wu_h, wu), (wd_h, wd)))
    ]
    for copy in weights:
        copy.start()

    barrier = pltpu.get_barrier_semaphore()
    for _, device in peers:
        pl.semaphore_signal(barrier, inc=1, device_id=device, device_id_type=pl.DeviceIdType.MESH)
    pl.semaphore_signal(barrier, inc=1, device_id=partner, device_id_type=pl.DeviceIdType.MESH)

    @pl.when(s < last)
    def _():
        for device in [above] + [{**d, **above} for _, d in far]:
            pl.semaphore_signal(barrier, inc=1, device_id=device, device_id_type=pl.DeviceIdType.MESH)

    @pl.when(s > 0)
    def _():
        for device in [below] + [{**d, **below} for _, d in far]:
            pl.semaphore_signal(barrier, inc=1, device_id=device, device_id_type=pl.DeviceIdType.MESH)

    with jax.named_scope("init_local"):
        for copy in inputs:
            copy.wait()
    links = (s < last).astype(jnp.int32) + (s > 0).astype(jnp.int32)
    with jax.named_scope("init_barrier"):
        pl.semaphore_wait(barrier, chips + (1 + len(far)) * links)

    my_cols = cols(block, bw)
    core_cols = cols(core, half)
    r15 = lambda ph, k: rbuf.at[ph, k, pl.ds(0, chips - 1)]

    def spread(ph, k, src, dst, targets):
        for _, device in targets:
            remote(src.at[k], dst.at[k, :, my_cols], ags.at[ph, k], agr.at[ph, k], device).start()
        dst[k, :, my_cols] = src[k]

    def hand_on(ph, k, src, dst, gathered, section):
        remote(src.at[k], dst.at[k], zs.at[ph, k], zr.at[ph, k], section).start()
        for _, device in far:
            remote(
                src.at[k], gathered.at[k, :, my_cols], zs.at[ph, k], agr.at[ph, k], {**device, **section}
            ).start()

    row_part = lambda k, c: rg.at[pl.ds(c * chips, chips), k]

    @pl.when(s == 0)
    def _():
        for k in range(micro):
            for _, device in peers:
                remote(tok.at[k], rg.at[block, k], xs.at[k], xr.at[k], device).start()
            rg[block, k] = tok[k]

    def forward_rows(k):
        most_rows = rg.at[pl.ds(0, chips - 1), k]
        remote(most_rows, most_rows, xs.at[k], xr.at[k], partner).wait_recv()
        remote(row_part(k, core), row_part(k, core), xds.at[k], xdr.at[k], partner).start()

    def place_rows(k):
        remote(row_part(k, other), row_part(k, other), xds.at[k], xdr.at[k], partner).wait_recv()
        for c in range(2):
            for n in range(chips):
                at = (n * 2 + c) * rows
                xg[k, at : at + rows, :] = rg[c * chips + n, k]

    chunk = min(512, half)
    gt_tab[...] = in_tab[...] * gain[...]
    acc_in[...] = jnp.zeros_like(acc_in)
    acc_out[...] = jnp.zeros_like(acc_out)
    gmid[...] = jnp.zeros_like(gmid)
    gtl[...] = jnp.zeros_like(gtl)
    i = lax.broadcasted_iota(jnp.int32, (total, total), 0)
    j = lax.broadcasted_iota(jnp.int32, (total, total), 1)
    i_mp = (i // (2 * rows)) % mps
    i_core = (i // rows) % 2
    source = (((i // (2 * rows * mps)) * 2 + i_core) * mps + i_mp) * rows + i % rows
    for k in range(micro):
        picked = jnp.where(source == j, jnp.broadcast_to(ids[k : k + 1, :], (total, total)), 0)
        idc[k] = jnp.sum(picked.astype(F32), axis=1, keepdims=True).astype(jnp.int32)
    for k in range(micro):
        for at in range(0, width, chunk):
            here = slice(at, at + chunk)
            in_rows[k, :, here] = pick(gt_tab[:, here], idc[k], members)
            out_rows[k, :, here] = pick(out_tab[:, here], idc[k], members)

    mine = pl.ds(core * micro, micro)
    first = remote(cot.at[:, :, cols(other, half)], t1.at[mine], isem.at[0], isem.at[1], partner)
    others = initr.at[pl.ds(0, chips - 1)]
    second = remote(others, others, isem.at[2], isem.at[3], partner)

    @pl.when(s == last)
    def _():
        first.start()
        t1[mine] = cot[:, :, cols(core, half)]
        first.wait_recv()
        for to, device in peers:
            remote(t1.at[:, :, cols(to, bw)], initr.at[q], isem.at[2], isem.at[3], device).start()
        initr[q] = t1[:, :, cols(q, bw)]
        second.wait_recv()
        for k in range(micro):
            for n in range(chips):
                for c in range(2):
                    at = (n * 2 + c) * rows
                    rowf[at : at + rows, :] = initr[n, c * micro + k].astype(F32)
            gin[k] = rowf[...].astype(BF16)
            spread(1, k, gin, gg, peers)

    with jax.named_scope("init_weights"):
        for copy in weights:
            copy.wait()

    pieces = [(at, min(256, hidden - at)) for at in range(0, hidden, 256)]

    def part_cols(c, n, size):
        return pl.ds(pl.multiple_of(c * half + n * size, size), size)

    def gathered(ph, k):
        remote(r15(ph, k), r15(ph, k), ags.at[ph, k], agr.at[ph, k], partner).wait_recv()

    def reduce_out(ph, k, term, between=None):
        step = min(512, half // 2)
        each = step // bw
        halves = half // 2 // step
        copies = []
        for piece in range(2):
            low = y_low if piece == 0 else 1 - y_low
            with jax.named_scope("down_other"):
                for n in range(halves):
                    at = other * half + low * (half // 2) + n * step
                    value = term(pl.ds(pl.multiple_of(at, step), step))
                    for e in range(each):
                        to = low * (chips // 2) + n * each + e
                        psend[ph, k, to] = value[:, e * bw : (e + 1) * bw].astype(BF16)
            at = pl.ds(low * (chips // 2), chips // 2)
            copy = remote(
                psend.at[ph, k, at], precv.at[ph, k, at], ps.at[ph, k, piece], pr.at[ph, k, piece], partner
            )
            copy.start()
            copies.append(copy)
        with jax.named_scope("down_own"):
            for n in range(half // step):
                value = term(pl.ds(pl.multiple_of(core * half + n * step, step), step))
                for e in range(each):
                    pf[n * each + e] = value[:, e * bw : (e + 1) * bw]
        if between is not None:
            between()
        for piece in range(2):
            low = y_low if piece == 0 else 1 - y_low
            with jax.named_scope("partner_wait"):
                copies[piece].wait_recv()
            with jax.named_scope("combine"):
                for n in range(chips // 2):
                    at = low * (chips // 2) + n
                    pown[ph, k, at] = (pf[at] + precv[ph, k, at].astype(F32)).astype(BF16)
                for to, device in groups[piece]:
                    remote(pown.at[ph, k, to], rbuf.at[ph, k, q], rs.at[ph, k], rr.at[ph, k], device).start()
        rbuf[ph, k, q] = pown[ph, k, q]

    def reduced(ph, k):
        with jax.named_scope("reduce_wait"):
            remote(r15(ph, k), r15(ph, k), rs.at[ph, k], rr.at[ph, k], partner).wait_recv()
        value = rbuf[ph, k, 0].astype(F32)
        for n in range(1, chips):
            value = value + rbuf[ph, k, n].astype(F32)
        return value

    def token_rows(k):
        return pl.ds(pl.multiple_of(k * total, total), total)

    def member_sums(acc, id_col, value):
        for m in range(members):
            acc[m : m + 1, :] += jnp.sum(jnp.where(id_col == m, value, 0.0), axis=0, keepdims=True)

    def fwd_arrive(k):
        with jax.named_scope("x_wait"):
            @pl.when(s > 0)
            def _():
                remote(xin.at[k], xin.at[k], zs.at[0, k], zr.at[0, k], above).wait_recv()
                spread(0, k, xin, xg, near)

            @pl.when(jnp.logical_and(s == 0, k == 0))
            def _():
                forward_rows(k)

    def fwd_compute(k):
        here = token_rows(k)
        id_col = idc[k]

        def scaled_half(c, squares):
            def step(n, carry):
                at = part_cols(c, n, chunk)
                x = xg[k, :, at].astype(F32)
                sc[here, at] = (x * in_rows[k, :, at]).astype(BF16)
                x2 = x * x
                for e in range(chunk // 128):
                    carry = carry + x2[:, e * 128 : (e + 1) * 128]
                return carry

            return lax.fori_loop(0, half // chunk, step, squares)

        part = xg.at[k, :, core_cols]
        copy = remote(part, part, ds.at[0, k], dr.at[0, k], partner)
        with jax.named_scope("gather_wait"):
            @pl.when(s > 0)
            def _():
                gathered(0, k)
                copy.start()

            @pl.when(s == 0)
            def _():
                place_rows(k)

        with jax.named_scope("gateup_own"):
            squares = scaled_half(core, jnp.zeros((total, 128), F32))
            at = core_cols
            for h, size in pieces:
                hs = slice(h, h + size)
                pacc[0, hs, :] = nt_dot(wg[hs, at], sc[here, at])
                pacc[1, hs, :] = nt_dot(wu[hs, at], sc[here, at])
        with jax.named_scope("forward_wait"):
            @pl.when(s > 0)
            def _():
                copy.wait_recv()
        with jax.named_scope("gateup_other"):
            squares = scaled_half(other, squares)
            scale = lax.rsqrt(jnp.sum(squares, axis=-1, keepdims=True) * (1.0 / width) + EPS)
            inv[k] = scale
            at = cols(other, half)
            for h, size in pieces:
                hs = slice(h, h + size)
                gate = (pacc[0, hs, :] + nt_dot(wg[hs, at], sc[here, at])).T * scale
                up = (pacc[1, hs, :] + nt_dot(wu[hs, at], sc[here, at])).T * scale
                gpre[k, :, hs] = gate
                upre[k, :, hs] = up
                product = gate / (1.0 + jnp.exp(-gate)) * up
                hid[here, hs] = (product * pick(mid_tab[:, hs], id_col, members)).astype(BF16)

    def fwd_down(k):
        @pl.when(jnp.logical_and(s == 0, k < micro - 1))
        def _():
            forward_rows(jnp.minimum(k + 1, micro - 1))

        h = hid[token_rows(k), :]
        reduce_out(0, k, lambda at: jnp.dot(h, wd[:, at], preferred_element_type=F32))

    def fwd_finish(k):
        value = reduced(0, k)
        with jax.named_scope("fwd_finish"):
            x = xg[k, :, my_cols].astype(F32)
            ob[k] = (x + value * out_rows[k, :, my_cols]).astype(BF16)

            @pl.when(s < last)
            def _():
                hand_on(0, k, ob, xin, xg, above)

            down[k] = value

    def bwd_arrive(k):
        with jax.named_scope("g_wait"):
            remote(gin.at[k], gin.at[k], zs.at[1, k], zr.at[1, k], below).wait_recv()
        with jax.named_scope("g_spread"):
            spread(1, k, gin, gg, near)

    def bwd_hidden(k):
        here = token_rows(k)

        def cot_half(c):
            def step(n, carry):
                at = part_cols(c, n, chunk)
                g = gg[k, :, at].astype(F32)
                ct[here, at] = (g * out_rows[k, :, at]).astype(BF16)
                return carry

            lax.fori_loop(0, half // chunk, step, 0)

        with jax.named_scope("g_gather_wait"):
            gathered(1, k)
            part = gg.at[k, :, core_cols]
            copy = remote(part, part, ds.at[1, k], dr.at[1, k], partner)
            copy.start()
        with jax.named_scope("hidden_own"):
            cot_half(core)
            at = core_cols
            for h, size in pieces:
                hs = slice(h, h + size)
                phid[k, hs, :] = nt_dot(wd[hs, at], ct[here, at])
        with jax.named_scope("g_forward_wait"):
            copy.wait_recv()
        with jax.named_scope("hidden_other"):
            cot_half(other)
            at = cols(other, half)
            for h, size in pieces:
                hs = slice(h, h + size)
                phid[k, hs, :] += nt_dot(wd[hs, at], ct[here, at])

    def bwd_compute(k):
        here = token_rows(k)
        id_col = idc[k]
        with jax.named_scope("grads"):
            scale = inv[k]
            dots = jnp.zeros((total, 1), F32)
            grad_pre = []
            grad_ups = []
            for h, size in pieces:
                hs = slice(h, h + size)
                grad_hidden = phid[k, hs, :].T
                gate = gpre[k, :, hs]
                up = upre[k, :, hs]
                sig = 1.0 / (1.0 + jnp.exp(-gate))
                silu = gate * sig
                grad_product = grad_hidden * pick(mid_tab[:, hs], id_col, members)
                grad_gate = grad_product * up * sig * (1.0 + gate * (1.0 - sig))
                grad_up = grad_product * silu
                ggate[:, hs] = grad_gate
                gup[:, hs] = grad_up
                gmids[:, hs] = grad_hidden * (silu * up)
                grad_gate = grad_gate.astype(BF16)
                grad_up = grad_up.astype(BF16)
                grad_pre.append(grad_gate)
                grad_ups.append(grad_up)
                dots = dots + jnp.sum(
                    grad_gate.astype(F32) * gate + grad_up.astype(F32) * up, axis=-1, keepdims=True
                )
            csend[k] = jnp.broadcast_to(dots, (total, 128)).T[0:1, :]
            ccopy = remote(csend.at[k], cprecv.at[k], cps.at[k], cpr.at[k], partner)
            ccopy.start()
            pre = jnp.concatenate(grad_pre + grad_ups, axis=1)

        def term(at):
            return jnp.dot(pre, wgu[:, at], preferred_element_type=F32)

        def send_dots():
            with jax.named_scope("dots"):
                ccopy.wait_recv()
                cown[k] = csend[k] + cprecv[k]
                for _, device in peers:
                    remote(cown.at[k], crbuf.at[k, q], cs.at[k], cr.at[k], device).start()
                crbuf[k, q] = cown[k]
            with jax.named_scope("keep"):
                dg[here, :] = (ggate[...] * scale).astype(BF16)
                du[here, :] = (gup[...] * scale).astype(BF16)
                member_sums(gmid, id_col, gmids[...])

        reduce_out(1, k, term, send_dots)

    def bwd_finish(k):
        id_col = idc[k]
        c15 = crbuf.at[k, pl.ds(0, chips - 1)]
        with jax.named_scope("dots_wait"):
            remote(c15, c15, cs.at[k], cr.at[k], partner).wait_recv()
            dots = crbuf[k, 0]
            for n in range(1, chips):
                dots = dots + crbuf[k, n]
            mean = jnp.broadcast_to(dots, (8, total)).T[:, 0:1] * (1.0 / width)
            scale = inv[k]
            g = gin[k].astype(F32)
            normed = xg[k, :, my_cols].astype(F32) * scale
            kept = g - scale * mean * normed
        grad_scaled = reduced(1, k)
        with jax.named_scope("bwd_finish"):
            grad_normed = grad_scaled * in_rows[k, :, my_cols]
            ig[k] = (kept + scale * grad_normed).astype(BF16)

            @pl.when(s > 0)
            def _():
                hand_on(1, k, ig, gin, gg, below)

            member_sums(acc_in, id_col, grad_scaled * normed)

    def out_scale_grad(k):
        member_sums(acc_out, idc[k], gin[k].astype(F32) * down[k])

    @pl.when(s == last)
    def _():
        lax.fori_loop(0, micro, lambda k, carry: (bwd_hidden(k), carry)[1], 0)

    behind = jnp.where(s == last, 0, micro + 2)
    down_behind = jnp.where(s == last, micro + 2, 1)

    def weight_grads():
        wide = min(1024, width)
        with jax.named_scope("weight_grads"):
            for left, right, out in ((dg, sc, g_gate), (du, sc, g_up), (hid, ct, g_down)):
                turned[...] = left[...].T

                def step(n, carry):
                    at = cols(n, wide)
                    out[:, at] = jnp.dot(turned[...], right[:, at], preferred_element_type=F32).astype(BF16)
                    return carry

                lax.fori_loop(0, width // wide, step, 0)

    def send_rows(kind, src):
        for k in range(micro):
            rowf[...] = src[k].astype(F32)
            for n in range(chips):
                for c in range(2):
                    at = (n * 2 + c) * rows
                    outs[kind, n, c * micro + k] = rowf[at : at + rows, :].astype(BF16)
        for to, device in peers:
            remote(
                outs.at[kind, to], outr.at[kind, :, :, cols(q, bw)],
                osem.at[kind], osem.at[2 + kind], device,
            ).start()
        outr[kind, :, :, cols(q, bw)] = outs[kind, q]

    def tick(t, carry):
        u = t - behind
        d = t - down_behind

        @pl.when(t < micro)
        def _():
            fwd_arrive(t)

        @pl.when(jnp.logical_and(s < last, jnp.logical_and(u >= 0, u < micro)))
        def _():
            bwd_arrive(u)

        @pl.when(jnp.logical_and(t >= 1, t < micro + 1))
        def _():
            fwd_compute(t - 1)

        @pl.when(jnp.logical_and(d >= 0, d < micro))
        def _():
            fwd_down(d)

        @pl.when(jnp.logical_and(s < last, jnp.logical_and(u >= 1, u < micro + 1)))
        def _():
            bwd_hidden(u - 1)

        @pl.when(jnp.logical_and(u >= 1, u < micro + 1))
        def _():
            bwd_compute(u - 1)

        @pl.when(jnp.logical_and(s == 0, u == micro + 1))
        def _():
            weight_grads()

        @pl.when(jnp.logical_and(d >= 1, d < micro + 1))
        def _():
            fwd_finish(d - 1)

        @pl.when(jnp.logical_and(s == last, jnp.logical_and(d >= 1, d < micro + 1)))
        def _():
            out_scale_grad(d - 1)

        @pl.when(d == micro)
        def _():
            send_rows(0, ob)

        @pl.when(jnp.logical_and(u >= 2, u < micro + 2))
        def _():
            bwd_finish(u - 2)

        @pl.when(jnp.logical_and(s < last, jnp.logical_and(u >= 2, u < micro + 2)))
        def _():
            out_scale_grad(u - 2)

        @pl.when(jnp.logical_and(s > 0, u == micro + 1))
        def _():
            weight_grads()

        return carry

    lax.fori_loop(0, 2 * (micro + 2), tick, 0)

    with jax.named_scope("end_send"):
        tables = acc_in[...]
        gtl[0:members, :] = tables * gain[:, my_cols]
        gtl[members : 2 * members, :] = acc_out[...]
        gtl[2 * members : 2 * members + 1, :] = jnp.sum(tables * in_tab[:, my_cols], axis=0, keepdims=True)
        gtab[:, my_cols] = gtl[...]
        for _, device in peers:
            remote(gtl, gtab.at[:, my_cols], osem.at[4], osem.at[5], device).start()
        send_rows(1, ig)

    with jax.named_scope("end_wait"):
        most = gtab.at[:, pl.ds(0, (chips - 1) * bw)]
        most_outs = [outs.at[kind, pl.ds(0, chips - 1)] for kind in range(2)]
        rows_on = [
            remote(
                outr.at[kind, pl.ds(other * micro, micro)], outp.at[kind],
                osem.at[6 + kind], osem.at[8 + kind], partner,
            )
            for kind in range(2)
        ]
        remote(most_outs[0], most_outs[0], osem.at[0], osem.at[2], partner).wait_recv()
        rows_on[0].start()
        remote(most, most, osem.at[4], osem.at[5], partner).wait_recv()
        table_part = gtab.at[:, core_cols]
        tables_on = remote(table_part, table_part, osem.at[10], osem.at[11], partner)
        tables_on.start()
        remote(most_outs[1], most_outs[1], osem.at[1], osem.at[3], partner).wait_recv()
        rows_on[1].start()
        out_x[:, :, core_cols] = outr[0, pl.ds(core * micro, micro)]
        out_g[:, :, core_cols] = outr[1, pl.ds(core * micro, micro)]

    with jax.named_scope("end_sent"):
        for k in range(micro):
            for ph in range(2):
                remote(r15(ph, k), r15(ph, k), rs.at[ph, k], rr.at[ph, k], partner).wait_send()
                part = psend.at[ph, k, pl.ds(0, chips // 2)]
                for piece in range(2):
                    remote(part, part, ps.at[ph, k, piece], pr.at[ph, k, piece], partner).wait_send()
            remote(csend.at[k], cprecv.at[k], cps.at[k], cpr.at[k], partner).wait_send()
            c15 = crbuf.at[k, pl.ds(0, chips - 1)]
            remote(c15, c15, cs.at[k], cr.at[k], partner).wait_send()
            half_x = xg.at[k, :, core_cols]
            near_x = rbuf.at[0, k, pl.ds(0, len(near))]
            far_x = rbuf.at[0, k, pl.ds(0, len(far) + 1)]
            remote(half_x, half_x, ds.at[1, k], dr.at[1, k], partner).wait_send()

            @pl.when(s == 0)
            def _():
                most_rows = rg.at[pl.ds(0, chips - 1), k]
                remote(most_rows, most_rows, xs.at[k], xr.at[k], partner).wait_send()
                remote(row_part(k, core), row_part(k, core), xds.at[k], xdr.at[k], partner).wait_send()

            @pl.when(s > 0)
            def _():
                remote(near_x, near_x, ags.at[0, k], agr.at[0, k], partner).wait_send()
                remote(half_x, half_x, ds.at[0, k], dr.at[0, k], partner).wait_send()
                remote(far_x, far_x, zs.at[1, k], zr.at[1, k], below).wait_send()

            @pl.when(s < last)
            def _():
                remote(near_x, near_x, ags.at[1, k], agr.at[1, k], partner).wait_send()
                remote(far_x, far_x, zs.at[0, k], zr.at[0, k], above).wait_send()

            @pl.when(s == last)
            def _():
                remote(r15(1, k), r15(1, k), ags.at[1, k], agr.at[1, k], partner).wait_send()

        @pl.when(s == last)
        def _():
            first.wait_send()
            second.wait_send()

        remote(most, most, osem.at[4], osem.at[5], partner).wait_send()
        for kind in range(2):
            remote(most_outs[kind], most_outs[kind], osem.at[kind], osem.at[2 + kind], partner).wait_send()
    with jax.named_scope("end_out"):
        tables_on.wait()
        g_in[...] = gtab[0:members, :]
        g_out[...] = gtab[members : 2 * members, :]
        g_gain[...] = gtab[2 * members : 2 * members + 1, :]
        rows_on[0].wait()
        out_x[:, :, cols(other, half)] = outp[0]
        rows_on[1].wait()
        out_g[:, :, cols(other, half)] = outp[1]


def deliver(count, *refs):
    sems = refs[-1]
    copies = [
        pltpu.make_async_copy(src, dst, sems.at[n])
        for n, (src, dst) in enumerate(zip(refs[:count], refs[count : 2 * count]))
    ]
    for copy in copies:
        copy.start()
    for copy in copies:
        copy.wait()


def on_device(
    tokens, member_ids, cotangent, w_gate, w_up, w_down, in_scale, mid_scale, out_scale, norm_gain
):
    sections = lax.axis_size("section")
    mps = lax.axis_size("mp")
    places = lax.axis_size("dp") // 2
    chips = places * mps
    micro, rows, width = tokens.shape
    total = member_ids.shape[1]
    members = in_scale.shape[1]
    hidden = w_gate.shape[2]
    half = width // 2
    bw = half // chips
    gate_t = w_gate[0].T
    up_t = w_up[0].T
    down_w = w_down[0]
    all_tokens = micro * total
    vmem = pl.BlockSpec(memory_space=pltpu.VMEM)
    hbm = pl.BlockSpec(memory_space=pl.ANY)
    dma = pltpu.SemaphoreType.DMA

    def buf(*shape, dtype=BF16):
        return pltpu.VMEM(shape, dtype)

    dims = (sections, places, mps, micro, rows, members)
    outs = (
        pltpu.VMEM((micro, rows, width), BF16),
        pltpu.VMEM((micro, rows, width), BF16),
        pltpu.VMEM((hidden, width), BF16),
        pltpu.VMEM((hidden, width), BF16),
        pltpu.VMEM((hidden, width), BF16),
        pltpu.VMEM((members, width), F32),
        pltpu.VMEM((members, width), F32),
        pltpu.VMEM((1, width), F32),
        pltpu.VMEM((members, hidden), F32),
    )
    results = pl.pallas_call(
        functools.partial(relay_kernel, dims),
        name="relay",
        out_shape=outs,
        in_specs=[pl.BlockSpec(memory_space=pltpu.HBM)] * 10,
        out_specs=[vmem] * len(outs),
        scratch_shapes=[
            buf(micro, rows, width), buf(micro, rows, width), buf(micro, total, dtype=jnp.int32),
            buf(members, width, dtype=F32), buf(1, width, dtype=F32),
            buf(members, width, dtype=F32), buf(members, hidden, dtype=F32),
            buf(micro, total, width, dtype=F32), buf(micro, total, width, dtype=F32),
            buf(all_tokens, hidden), buf(all_tokens, hidden), buf(all_tokens, hidden),
            buf(all_tokens, width), buf(all_tokens, width), buf(hidden, all_tokens),
            buf(total, hidden, dtype=F32), buf(total, hidden, dtype=F32), buf(total, hidden, dtype=F32),
            buf(2 * hidden, width), buf(hidden, width),
            buf(2 * chips, micro, rows, width),
            buf(2 * micro, rows, half),
            buf(chips, 2 * micro, rows, bw),
            buf(total, bw, dtype=F32),
            buf(micro, total, bw), buf(micro, total, bw),
            buf(micro, total, width), buf(micro, total, width),
            buf(members, width, dtype=F32),
            buf(micro, total, 1, dtype=jnp.int32),
            buf(micro, total, 1, dtype=F32),
            buf(2, hidden, total, dtype=F32), buf(micro, hidden, total, dtype=F32),
            buf(micro, total, hidden, dtype=F32), buf(micro, total, hidden, dtype=F32),
            buf(2, micro, chips, total, bw), buf(2, micro, chips, total, bw),
            buf(2, micro, chips, total, bw),
            buf(chips, total, bw, dtype=F32),
            buf(2, micro, chips, total, bw),
            buf(micro, 1, total, dtype=F32), buf(micro, 1, total, dtype=F32),
            buf(micro, 1, total, dtype=F32), buf(micro, chips, 1, total, dtype=F32),
            buf(micro, total, bw, dtype=F32),
            buf(micro, total, bw), buf(micro, total, bw),
            buf(members, bw, dtype=F32), buf(members, bw, dtype=F32),
            buf(16, bw, dtype=F32), buf(16, width, dtype=F32),
            buf(2, chips, 2 * micro, rows, bw),
            buf(2, 2 * micro, rows, half),
            buf(2, micro, rows, half),
            dma((7,)), dma((3,)), dma((4,)),
            dma((micro,)), dma((micro,)), dma((micro,)), dma((micro,)),
            dma((2, micro)), dma((2, micro)), dma((2, micro)), dma((2, micro)),
            dma((2, micro)), dma((2, micro)), dma((2, micro, 2)), dma((2, micro, 2)),
            dma((2, micro)), dma((2, micro)),
            dma((micro,)), dma((micro,)), dma((micro,)), dma((micro,)),
            dma((12,)),
        ],
        compiler_params=pltpu.CompilerParams(
            collective_id=0, has_side_effects=True, vmem_limit_bytes=46 * 1024 * 1024
        ),
    )(
        tokens, cotangent, member_ids, in_scale[0], norm_gain, out_scale[0], mid_scale[0],
        gate_t, up_t, down_w,
    )

    out_x, out_g, grad_gate, grad_up, grad_down, g_in, g_out, g_gain, gmid = pl.pallas_call(
        functools.partial(deliver, len(outs)),
        name="deliver",
        out_shape=[jax.ShapeDtypeStruct(o.shape, o.dtype) for o in outs],
        in_specs=[vmem] * len(outs),
        out_specs=[hbm] * len(outs),
        scratch_shapes=[dma((len(outs),))],
        compiler_params=pltpu.CompilerParams(vmem_limit_bytes=1024 * 1024),
    )(*[pltpu.with_memory_space_constraint(r, pltpu.VMEM) for r in results])

    return (
        out_x[None],
        out_g[None],
        grad_gate.T[None],
        grad_up.T[None],
        grad_down[None],
        g_in[None],
        gmid[None],
        g_out[None],
        g_gain,
    )


def solution(mesh):
    in_specs = (
        P(None, ("dp", "mp"), None),
        P(),
        P(None, ("dp", "mp"), None),
        P("section", None, ("dp", "mp")),
        P("section", None, ("dp", "mp")),
        P("section", ("dp", "mp"), None),
        P("section", None, None),
        P("section", None, ("dp", "mp")),
        P("section", None, None),
        P("section", None),
    )
    out_specs = (
        P("section", None, ("dp", "mp"), None),
        P("section", None, ("dp", "mp"), None),
        P("section", None, ("dp", "mp")),
        P("section", None, ("dp", "mp")),
        P("section", ("dp", "mp"), None),
        P("section", None, None),
        P("section", None, ("dp", "mp")),
        P("section", None, None),
        P("section", None),
    )
    return jax.shard_map(
        on_device, mesh=mesh, in_specs=in_specs, out_specs=out_specs, check_vma=False
    )
```
